256 devices in a mesh: gz: 2 (over core), gx: 16 (over y, x), gy: 8 (over z).
Axes of the slice: x: 4, y: 4, z: 8, core: 2. Of those that a mesh axis runs over, the one named last changes fastest.
Arguments:
- positions: float32 [128, 3, 65536], P(('gz', 'gy'), None, 'gx'), may hold values from -8 to 8
- diffusion_noise: float32 [128, 3, 65536], P(('gz', 'gy'), None, 'gx'), may hold values from -5 to 5
- base_nuclei: float32 [16, 3], replicated, may hold values from -4.15 to 4.15, as said below
- displacements: float32 [8, 16, 3], replicated, may hold values from -0.4375 to 0.4375
- charges: float32 [16], replicated, may hold values from 2 to 14
- orbital_decay: float32 [16], replicated, may hold values from 0.6 to 2
- coefficients: float32 [16], replicated, may hold values from 0.5 to 2
- weights: float32 [65536], P('gx'), may hold values from 0.5 to 2
- counts: int32 [512], P('gx'), may hold values from 1 to 128
- branch_source: int32 [512], replicated, may hold values from 0 to 511, as said below
Outputs:
- local_energy: float32 [8, 65536], P('gz', 'gx')
- energy_estimate: float32 [8], P('gz')
- new_positions: float32 [128, 3, 65536], P(('gz', 'gy'), None, 'gx')
- new_weights: float32 [65536], P('gx')
The draws below stay inside these ranges and needn't reach their ends.
Inputs may be any that keep to these rules, and one draw needn't show every extreme that they name: `branch_source`: A permutation of the blocks. Of the 32 destination blocks of each aligned group (d // 32 equal), at most 4 have sources in any one aligned group of 32 source blocks, and some pair reaches 4 for every group, as sender and as receiver. `base_nuclei`: any two nuclei lie 1.7 or more apart.
All inputs are finite; a program needn't handle non-finite values.
Results may differ from the reference program's by a relative error of at most 0.0002.
Values sent between devices are 32-bit elements; how exact they have to be, the bound alone decides.
A program may use at most 64 MiB of HBM per device.

```python
import math
import jax
import jax.numpy as jnp
from jax import lax

NE = 128
NA = 16
BLK = 128
G = 8
W = 65536
NBLK = 512
BPD = 32
CAP = 4
N_GX = 16


def draw_base_nuclei(key, part):
    atoms = jnp.arange(NA, dtype=jnp.int32)
    lattice = jnp.stack([atoms % 4, atoms // 4 % 2, atoms // 8], axis=1).astype(jnp.float32) * 2.5
    lattice = lattice - jnp.array([3.75, 1.25, 1.25], dtype=jnp.float32)
    jitter = jax.random.uniform(jax.random.fold_in(key, 11), (NA, 3), jnp.float32, -0.4, 0.4)
    return (lattice + jitter).astype(jnp.float32)


def draw_branch_source(key, part):
    key_sigma = jax.random.fold_in(key, 21)
    key_shift = jax.random.fold_in(key, 22)
    key_order = jax.random.fold_in(key, 23)
    key_slots = jax.random.fold_in(key, 24)
    peers = N_GX
    ranking = jax.random.permutation(key_sigma, peers).astype(jnp.int32) + 3
    ranking = ranking.at[peers // 2].set(0).at[0].set(1).at[1].set(2)
    sigma = jnp.argsort(ranking, stable=True).astype(jnp.int32)
    sigma_inverse = jnp.argsort(sigma).astype(jnp.int32)
    offsets = jnp.arange(peers, dtype=jnp.int32)
    filled = BPD // CAP
    amounts = jnp.where(offsets < filled, CAP, 0).astype(jnp.int32)
    if filled >= 2 and filled < peers:
        moving = jax.random.randint(key_shift, (), 0, CAP).astype(jnp.int32)
        amounts = amounts.at[filled - 1].add(-moving).at[filled].add(moving)
    offset_list = jnp.repeat(offsets, amounts, total_repeat_length=BPD)
    source_device = jnp.broadcast_to(offsets[:, None], (peers, BPD))
    destination = sigma[(sigma_inverse[source_device] + 1 + offset_list[None, :]) % peers]
    local_order = jax.vmap(lambda part_key: jax.random.permutation(part_key, BPD))(jax.random.split(key_order, peers)).astype(jnp.int32)
    source_block = source_device * BPD + local_order
    sort_keys = destination * NBLK + jax.random.permutation(key_slots, NBLK).astype(jnp.int32).reshape(peers, BPD)
    ordering = jnp.argsort(sort_keys.reshape(-1), stable=True)
    return source_block.reshape(-1)[ordering].astype(jnp.int32)


def plant(entries, own_key, least, top_value):
    longest = entries.shape.index(max(entries.shape))
    spots = []
    for shift in (0, 1):
        where = [jax.random.randint(jax.random.fold_in(own_key, axis), (), 0, length) for axis, length in enumerate(entries.shape)]
        where[longest] = (where[longest] + shift) % entries.shape[longest]
        spots.append(tuple(where))
    return entries.at[spots[0]].set(least).at[spots[1]].set(top_value)


def block_levels(own_key, extent, cuts, least, largest):
    loudness = 1.0
    for axis_at, shards_of in cuts:
        draws = jax.random.uniform(jax.random.fold_in(jax.random.fold_in(own_key, 6), axis_at), (shards_of,), jnp.float32, least / len(cuts), largest / len(cuts))
        loudness = loudness * jnp.repeat(jnp.exp(draws), extent[axis_at] // shards_of).reshape((-1,) + (1,) * (len(extent) - 1 - axis_at))
    return loudness


def normal_values(key, extent, spread, bound, cuts=(), kind=jnp.bfloat16):
    result = spread * jax.random.normal(key, extent, jnp.float32)
    if cuts:
        result = result * block_levels(key, extent, cuts, -0.22, 0.18)
    return jnp.clip(result, -bound, bound).astype(kind)


def setup_inputs(seed: int = 0) -> dict:
    streams_of = jax.random.split(jax.random.key(seed), 11)
    positions = normal_values(streams_of[0], (NE, 3, W), 2.0, 8.0, ((0, 16), (2, 16)), jnp.float32)
    diffusion_noise = normal_values(streams_of[1], (NE, 3, W), 1.0, 5.0, ((0, 16), (2, 16)), jnp.float32)
    base_nuclei = draw_base_nuclei(jax.random.fold_in(streams_of[10], 71), 0)
    displacements = normal_values(streams_of[3], (G, NA, 3), 0.03, 0.4375, (), jnp.float32)
    charges = jnp.clip(jnp.exp(jax.random.uniform(streams_of[4], (NA,), jnp.float32, math.log(2.0), math.log(14.0))), 2.0, 14.0)
    orbital_decay = jnp.clip(jnp.exp(jax.random.uniform(streams_of[5], (NA,), jnp.float32, math.log(0.6), math.log(2.0))), 0.6, 2.0)
    coefficients = jnp.clip(jnp.exp(jax.random.uniform(streams_of[6], (NA,), jnp.float32, math.log(0.5), math.log(2.0))), 0.5, 2.0)
    weights = jnp.clip(jnp.exp(math.log(2.0) - 1.3862944 * jax.random.uniform(streams_of[7], (W,), jnp.float32) ** block_levels(streams_of[7], (W,), ((0, 16),), -0.2, 0.2)), 0.5, 2.0)
    counts = plant(jax.random.randint(streams_of[8], (NBLK,), 1, BLK + 1), jax.random.fold_in(streams_of[8], 1), 1, BLK).astype(jnp.int32)
    branch_source = draw_branch_source(jax.random.fold_in(streams_of[10], 71), 0)
    return dict(positions=positions, diffusion_noise=diffusion_noise, base_nuclei=base_nuclei, displacements=displacements, charges=charges, orbital_decay=orbital_decay, coefficients=coefficients, weights=weights, counts=counts, branch_source=branch_source)


soft_square = 0.04
cusp_value = 0.5
jastrow_range = 1.0
time_step = 0.01
step_root = 0.1

def orbital_terms(coords, centers, charges, orbital_decay, coefficients):
    offsets = coords[:, None, :, :] - centers[None, :, :, None]
    square_dist = lax.optimization_barrier(jnp.sum(offsets * offsets, axis=2))
    distance = jnp.sqrt(square_dist + soft_square)
    decay = orbital_decay[None, :, None]
    orbital_part = coefficients[None, :, None] * jnp.exp(-decay * distance)
    orbital = lax.optimization_barrier(jnp.sum(orbital_part, axis=1))
    grad_orbital = lax.optimization_barrier(jnp.sum((-decay * orbital_part / distance)[:, :, None, :] * offsets, axis=1))
    lap_orbital = lax.optimization_barrier(jnp.sum(orbital_part * (decay * decay * square_dist / (distance * distance) - decay * (2.0 * distance * distance + soft_square) / (distance * distance * distance)), axis=1))
    grad_log = grad_orbital / orbital[:, None, :]
    potential = -lax.optimization_barrier(jnp.sum(charges[None, :, None] / distance, axis=1))
    return (jnp.log(orbital), grad_log, lap_orbital / orbital, potential)

def pair_terms(coords, others, coord_index, other_index):
    offsets = coords[:, None, :, :] - others[None, :, :, :]
    square_dist = lax.optimization_barrier(jnp.sum(offsets * offsets, axis=2))
    distance = jnp.sqrt(square_dist + soft_square)
    keeping = (coord_index[:, None] != other_index[None, :]).astype(jnp.float32)[:, :, None]
    denominator = 1.0 + jastrow_range * distance
    slope = keeping * cusp_value / (denominator * denominator)
    bending = keeping * (-2.0 * cusp_value * jastrow_range) / (denominator * denominator * denominator)
    gradient = lax.optimization_barrier(jnp.sum((slope / distance)[:, :, None, :] * offsets, axis=1))
    laplacian = lax.optimization_barrier(jnp.sum(bending * square_dist / (distance * distance) + slope * (2.0 * distance * distance + soft_square) / (distance * distance * distance), axis=1))
    coulomb = 0.5 * lax.optimization_barrier(jnp.sum(keeping / distance, axis=1))
    return (gradient, laplacian, coulomb)

def nuclear_repulsion(centers, charges):
    offsets = centers[:, None, :] - centers[None, :, :]
    identity = jnp.eye(centers.shape[0], dtype=jnp.float32)
    distance = jnp.sqrt(lax.optimization_barrier(jnp.sum(offsets * offsets, axis=2)) + identity)
    return 0.5 * jnp.sum(charges[:, None] * charges[None, :] * (1.0 - identity) / distance)

def electron_energy(grad_log, laplace_ratio, potential, jgrad, jlap, coulomb):
    total_grad = grad_log + jgrad
    kinetic = -0.5 * (laplace_ratio - lax.optimization_barrier(jnp.sum(grad_log * grad_log, axis=1)) + jlap + lax.optimization_barrier(jnp.sum(total_grad * total_grad, axis=1)))
    return kinetic + potential + coulomb

def reference(positions, diffusion_noise, base_nuclei, displacements, charges, orbital_decay, coefficients, weights, counts, branch_source):
    centers = base_nuclei[None, :, :] + displacements
    block_coords = positions.reshape(NE, 3, NBLK, BLK).transpose(2, 0, 1, 3)
    electron_index = jnp.arange(NE, dtype=jnp.int32)

    def walker_block(coords):
        jgrad, jlap, coulomb = pair_terms(coords, coords, electron_index, electron_index)
        energies = []
        log_sums = []
        drifted = coords
        for geometry in range(G):
            log_orbital, grad_log, laplace_ratio, potential = orbital_terms(coords, centers[geometry], charges, orbital_decay, coefficients)
            energies.append(lax.optimization_barrier(jnp.sum(electron_energy(grad_log, laplace_ratio, potential, jgrad, jlap, coulomb), axis=0)))
            log_sums.append(lax.optimization_barrier(jnp.sum(log_orbital, axis=0)))
            if geometry == 0:
                drifted = coords + time_step * (grad_log + jgrad)
        return (jnp.stack(energies), jnp.stack(log_sums), drifted)
    energy_blocks, log_blocks, drift_blocks = lax.map(walker_block, block_coords)
    energies = energy_blocks.transpose(1, 0, 2).reshape(G, W)
    log_sums = log_blocks.transpose(1, 0, 2).reshape(G, W)
    drifted = drift_blocks.transpose(1, 2, 0, 3).reshape(NE, 3, W)
    nuclear_energy = jnp.stack([nuclear_repulsion(centers[geometry], charges) for geometry in range(G)])
    local_energy = (energies + nuclear_energy[:, None]) / NE
    alive_mask = (jnp.arange(BLK, dtype=jnp.int32)[None, :] < counts[:, None]).astype(jnp.float32).reshape(W)
    weight_ratio = jnp.exp(2.0 * (log_sums - log_sums[0:1]))
    sample_weight = weights[None, :] * weight_ratio * alive_mask[None, :]
    energy_estimate = lax.optimization_barrier(jnp.sum(sample_weight * local_energy, axis=1)) / lax.optimization_barrier(jnp.sum(sample_weight, axis=1))
    kept_weights = alive_mask * weights * jnp.exp(-(local_energy[0] - energy_estimate[0]))
    moved_positions = drifted + step_root * diffusion_noise
    new_positions = moved_positions.reshape(NE, 3, NBLK, BLK)[:, :, branch_source].reshape(NE, 3, W)
    new_weights = kept_weights.reshape(NBLK, BLK)[branch_source].reshape(W)
    return (local_energy, energy_estimate, new_positions, new_weights)
```

```python
import functools
import math

import jax
import jax.numpy as jnp
from jax import lax
from jax.experimental import pallas as pl
from jax.experimental.pallas import tpu as pltpu
from jax.sharding import Mesh
from jax.sharding import PartitionSpec as P

NE = 128
BLK = 128
GX = ("gx_0", "gx_1")


soft_square = 0.04
cusp_value = 0.5
jastrow_range = 1.0
time_step = 0.01
step_root = 0.1


def in_blocks(x, dim, peers):
    shape = x.shape
    parts = x.reshape(*shape[:dim], peers, shape[dim] // peers, *shape[dim + 1 :])
    return jnp.moveaxis(parts, dim, 0)


def laid_out(parts, dim):
    shape = list(parts.shape[1:])
    shape[dim] *= parts.shape[0]
    return jnp.moveaxis(parts, 0, dim).reshape(shape)


def turned_blocks(parts, axes, sequence):
    inside = parts.shape[1:]
    out = parts.reshape(*(lax.axis_size(a) for a in axes), *inside)
    for k in sequence:
        out = lax.all_to_all(out, axes[k], k, k, tiled=True)
    return out.reshape(-1, *inside)


def one_axis_at_a_time(x, axes, sequence, split_dim, concat_dim):
    parts = in_blocks(x, split_dim, lax.axis_size(axes))
    return laid_out(turned_blocks(parts, axes, sequence), concat_dim)


def sent_together(arrays, axis, dim, along):
    widths = [a.shape[along] for a in arrays]
    both = jnp.concatenate(arrays, axis=along)
    out = lax.all_gather(both, axis, axis=dim, tiled=True)
    return tuple(jnp.split(out, [sum(widths[:k]) for k in range(1, len(widths))], axis=along))


def over_axes(x, axes):
    return functools.reduce(lax.psum, axes, x)


def side_by_side(arrays, axis, split_dim, concat_dim, along):
    ends, at = ([], 0)
    for a in arrays[:-1]:
        at += a.shape[along]
        ends.append(at)
    both = jnp.concatenate(arrays, axis=along)
    return tuple(
        jnp.split(
            lax.all_to_all(both, axis, split_axis=split_dim, concat_axis=concat_dim, tiled=True),
            ends,
            axis=along,
        )
    )


NA = 16
G = 8
f32 = jnp.float32
LOG2E=math.log2(math.e)

def prep_consts(base, disp, charges, decay, coef):
    centers=(base[None]+disp)*5.0
    a=decay*0.2
    ga=lambda v: jnp.broadcast_to(v[None,:],(G,NA))
    rows=jnp.stack([centers[...,0],centers[...,1],centers[...,2],ga(-a*LOG2E),ga(coef),ga(a),ga(a*a),ga(charges)])
    return rows.reshape(8,G*NA)

PAD=8
def pair_phase(h, pbuf, jacc, grad, U=8):
    zero=jnp.zeros((8,128),f32)
    def itile(I,carry):
        r0=pl.multiple_of(I*8,8)
        xi=pbuf[h,0,pl.ds(r0,8),:];yi=pbuf[h,1,pl.ds(r0,8),:];zi=pbuf[h,2,pl.ds(r0,8),:]
        def one(base,s,acc,keep=None):
            gx,gy,gz,lap,co=acc
            row=base+s
            dx=xi-pbuf[h,0,pl.ds(row,8),:];dy=yi-pbuf[h,1,pl.ds(row,8),:];dz=zi-pbuf[h,2,pl.ds(row,8),:]
            d2=(dx*dx+1.0)+(dy*dy+dz*dz)
            r=lax.rsqrt(d2)
            m=d2*r+5.0
            t=lax.rsqrt(m*m)
            c=t*t*r
            b=t*(r+5.0)+0.5*(r*r)
            if keep is not None:
                c=c*keep; r=r*keep
            cx=c*dx;cy=c*dy;cz=c*dz
            bb=pl.multiple_of(base+PAD,8)
            jacc[s,0,pl.ds(bb,8),:]+=cx
            jacc[s,1,pl.ds(bb,8),:]+=cy
            jacc[s,2,pl.ds(bb,8),:]+=cz
            return (gx+cx,gy+cy,gz+cz,lap+c*b,co+r)
        def mloop(mm,acc):
            base=pl.multiple_of(r0+mm*8,8)
            for s in range(8):
                acc=one(base,s,acc)
            return acc
        acc=(zero,zero,zero,carry[0],carry[1])
        for s in range(1,8):
            acc=one(r0,s,acc)
        acc=lax.fori_loop(1,8,mloop,acc)
        keep=jnp.where(I<8,jnp.float32(1),jnp.float32(0))
        acc=one(pl.multiple_of(r0+64,8),0,acc,keep)
        for c in range(3):
            grad[h,c,pl.ds(r0,8),:]=acc[c]
        return acc[3],acc[4]
    lap,co=lax.fori_loop(0,16,itile,(zero,zero))
    def fold(I,jj):
        r0=pl.multiple_of(I*8,8)
        for c in range(3):
            g=grad[h,c,pl.ds(r0,8),:]
            for s in range(8):
                g=g-jacc[s,c,pl.ds(r0+(PAD-s),8),:]
                g=g-jacc[s,c,pl.ds(r0+(PAD-s)+128,8),:]
            grad[h,c,pl.ds(r0,8),:]=g
            jj=jj+g*g
        return jj
    jj=lax.fori_loop(0,16,fold,zero)
    return -125.0*lap+5.0*co-78.125*jj

def bc(k_ref,i,row):
    return jnp.full((8,128),k_ref[i,row],f32)

def orbital_phase(g, pbuf, grad, k_ref, esum, lsum, drift_ref, T=4):
    zero=jnp.zeros((8,128),f32)
    for h in range(2):
        def group(q,acc):
            en,lg=acc
            rows=[pl.multiple_of(q*(8*T)+8*i,8) for i in range(T)]
            ph=[zero]*T;gx=[zero]*T;gy=[zero]*T;gz=[zero]*T;la=[zero]*T;po=[zero]*T
            for a in range(NA):
                row=g*NA+a
                cx,cy,cz,na,co,al,a2,ch=[k_ref[i,row] for i in range(8)]
                for i in range(T):
                    vx=pbuf[h,0,pl.ds(rows[i],8),:]-cx
                    vy=pbuf[h,1,pl.ds(rows[i],8),:]-cy
                    vz=pbuf[h,2,pl.ds(rows[i],8),:]-cz
                    d2=(vx*vx+1.0)+(vy*vy+vz*vz)
                    r=lax.rsqrt(d2)
                    d=d2*r
                    e=co*jnp.exp2(na*d)
                    w=e*(al*r)
                    t2=r*(r+al)+2.0
                    ph[i]=ph[i]+e
                    gx[i]=gx[i]+w*vx
                    gy[i]=gy[i]+w*vy
                    gz[i]=gz[i]+w*vz
                    la[i]=la[i]+(a2*e-w*t2)
                    po[i]=po[i]+ch*r
            for i in range(T):
                inv=1.0/ph[i]
                jx=grad[h,0,pl.ds(rows[i],8),:];jy=grad[h,1,pl.ds(rows[i],8),:];jz=grad[h,2,pl.ds(rows[i],8),:]
                dot=gx[i]*jx+gy[i]*jy+gz[i]*jz
                en=en+(62.5*dot-12.5*la[i])*inv-5.0*po[i]
                lg=lg+jnp.log(ph[i])
                if drift_ref is not None:
                    for c,(gg,jj) in enumerate(((gx[i],jx),(gy[i],jy),(gz[i],jz))):
                        p=pbuf[h,c,pl.ds(rows[i],8),:]*0.2
                        drift_ref[c,pl.ds(rows[i],8),h*128:(h+1)*128]=p+(0.125*jj-(0.05*gg)*inv)
            return en,lg
        en,lg=lax.fori_loop(0,NE//(8*T),group,(zero,zero))
        esum[h,g]=en
        lsum[h,g]=lg

def compute_kernel(pos_ref, k_ref, drift_ref, e_ref, l_ref, pbuf, jacc, grad, esum, lsum, *, do_pair=True, do_orb=True):
    for h in range(2):
        for c in range(3):
            p=pos_ref[c,:,h*128:(h+1)*128]*5.0
            pbuf[h,c,0:128,:]=p
            pbuf[h,c,128:256,:]=p
    base=[]
    for h in range(2):
        if do_pair:
            def zr(i,_):
                for s in range(8):
                    for c in range(3):
                        jacc[s,c,pl.ds(pl.multiple_of(i*8,8),8),:]=jnp.zeros((8,128),f32)
                return 0
            lax.fori_loop(0,34,zr,0)
            base.append(pair_phase(h,pbuf,jacc,grad))
        else:
            base.append(jnp.zeros((8,128),f32))
    if do_orb:
        orbital_phase(0,pbuf,grad,k_ref,esum,lsum,drift_ref)
        def gl(g,_):
            orbital_phase(g,pbuf,grad,k_ref,esum,lsum,None)
            return 0
        lax.fori_loop(1,G,gl,0)
    for h in range(2):
        for g in range(G):
            e_ref[g:g+1,h*128:(h+1)*128]=jnp.sum(esum[h,g]+base[h],axis=0,keepdims=True)
            l_ref[g:g+1,h*128:(h+1)*128]=jnp.sum(lsum[h,g],axis=0,keepdims=True)

def scratch():
    return [pltpu.VMEM((2,3,256,128),f32),pltpu.VMEM((8,3,34*8,128),f32),pltpu.VMEM((2,3,128,128),f32),
            pltpu.VMEM((2,G,8,128),f32),pltpu.VMEM((2,G,8,128),f32)]

def compute(pos3, consts, **kw):
    return pl.pallas_call(functools.partial(compute_kernel,**kw),
        out_shape=(jax.ShapeDtypeStruct((3,NE,256),f32),jax.ShapeDtypeStruct((G,256),f32),jax.ShapeDtypeStruct((G,256),f32)),
        in_specs=[pl.BlockSpec(memory_space=pltpu.VMEM),pl.BlockSpec(memory_space=pltpu.SMEM)],
        out_specs=(pl.BlockSpec(memory_space=pltpu.VMEM),)*3,
        scratch_shapes=scratch(),
        compiler_params=pltpu.CompilerParams(vmem_limit_bytes=40*2**20),
        )(pos3,consts)


def nuclear_repulsion(centers, charges):
    offsets = centers[:, None, :] - centers[None, :, :]
    identity = jnp.eye(centers.shape[0], dtype=jnp.float32)
    distance = jnp.sqrt(jnp.sum(offsets * offsets, axis=2) + identity)
    return 0.5 * jnp.sum(charges[:, None] * charges[None, :] * (1.0 - identity) / distance)


def local(
    positions,
    diffusion_noise,
    base_nuclei,
    displacements,
    charges,
    orbital_decay,
    coefficients,
    weights,
    counts,
    branch_source,
):
    own_count = positions.shape[0]
    walkers = positions.shape[2]
    geometries = displacements.shape[0]
    per_replica = geometries // lax.axis_size("gz")
    replica = lax.axis_index("gz")
    centers = base_nuclei[None, :, :] + displacements
    whole_walkers = one_axis_at_a_time(positions, ("gz", "gy"), (0, 1), 2, 0)
    drift3, energies, log_sums = compute(
        whole_walkers.transpose(1, 0, 2),
        prep_consts(base_nuclei, displacements, charges, orbital_decay, coefficients),
    )
    drift_whole = drift3.transpose(1, 0, 2)
    energies, log_sums = sent_together((energies, log_sums), ("gz", "gy"), 1, 0)
    drifted = lax.all_to_all(drift_whole, ("gz", "gy"), split_axis=0, concat_axis=2, tiled=True)
    energies = jnp.concatenate(
        [lax.dynamic_slice_in_dim(energies, replica * per_replica, per_replica, 0), energies[0:1]],
        axis=0,
    )
    log_sums = jnp.concatenate(
        [lax.dynamic_slice_in_dim(log_sums, replica * per_replica, per_replica, 0), log_sums[0:1]],
        axis=0,
    )
    chosen_centers = jnp.concatenate(
        [lax.dynamic_slice_in_dim(centers, replica * per_replica, per_replica, 0), centers[0:1]],
        axis=0,
    )
    nuclear_energy = jnp.stack(
        [
            nuclear_repulsion(chosen_centers[geometry], charges)
            for geometry in range(per_replica + 1)
        ]
    )
    local_energy = (energies + nuclear_energy[:, None]) / NE
    alive_mask = (
        (jnp.arange(BLK, dtype=jnp.int32)[None, :] < counts[:, None])
        .astype(jnp.float32)
        .reshape(walkers)
    )
    weight_ratio = jnp.exp(2.0 * (log_sums - log_sums[-1:]))
    sample_weight = weights[None, :] * weight_ratio * alive_mask[None, :]
    numerator, denominator = (
        over_axes(jnp.sum(sample_weight * local_energy, axis=1), GX),
        over_axes(jnp.sum(sample_weight, axis=1), GX),
    )
    estimate = numerator / denominator
    kept_weights = alive_mask * weights * jnp.exp(-(local_energy[-1] - estimate[-1]))
    moved_positions = drifted + step_root * diffusion_noise
    blocks_here = counts.shape[0]
    block_total = branch_source.shape[0]
    device = lax.axis_index(GX)
    coord_blocks = moved_positions.reshape(own_count * 3, blocks_here, BLK)
    weight_blocks = kept_weights.reshape(1, blocks_here, BLK)
    my_sources = lax.dynamic_slice_in_dim(branch_source, device * blocks_here, blocks_here, 0)
    peers = lax.axis_size(GX)
    capacity = max(2, 2 * blocks_here // peers)
    block_range = jnp.arange(blocks_here, dtype=jnp.int32)
    own_ids = device * blocks_here + block_range
    matches = (branch_source[None, :] == own_ids[:, None]).astype(jnp.int32)
    dest_slot = jnp.sum(matches * jnp.arange(block_total, dtype=jnp.int32)[None, :], axis=1)
    dest_device = dest_slot // blocks_here
    earlier = (
        (dest_device[None, :] == dest_device[:, None]) & (dest_slot[None, :] < dest_slot[:, None])
    ).astype(jnp.int32)
    send_slot = dest_device * capacity + jnp.sum(earlier, axis=1)
    selection = (
        jnp.arange(peers * capacity, dtype=jnp.int32)[:, None] == send_slot[None, :]
    ).astype(jnp.int32)
    picked = jnp.sum(selection * block_range[None, :], axis=1)
    occupied = jnp.sum(selection, axis=1).astype(jnp.float32)
    send_coords = jnp.take(coord_blocks, picked, axis=1) * occupied[None, :, None]
    send_weights = jnp.take(weight_blocks, picked, axis=1) * occupied[None, :, None]
    recv_coords, recv_weights = side_by_side((send_coords, send_weights), GX, 1, 1, 0)
    source_device = my_sources // blocks_here
    before = (
        (source_device[None, :] == source_device[:, None])
        & (block_range[None, :] < block_range[:, None])
    ).astype(jnp.int32)
    slot_index = source_device * capacity + jnp.sum(before, axis=1)
    new_coords = jnp.take(recv_coords, slot_index, axis=1)
    new_weight_blocks = jnp.take(recv_weights, slot_index, axis=1)
    new_positions = new_coords.reshape(own_count, 3, walkers)
    new_weights = new_weight_blocks.reshape(walkers)
    return (local_energy[:-1], estimate[:-1], new_positions, new_weights)


def solution(mesh):
    split = Mesh(
        mesh.devices.reshape(mesh.shape["gz"], 4, 4, mesh.shape["gy"]), ("gz", "gx_0", "gx_1", "gy")
    )
    placed = (
        P(("gz", "gy"), None, GX),
        P(("gz", "gy"), None, GX),
        P(),
        P(),
        P(),
        P(),
        P(),
        P(GX),
        P(GX),
        P(),
    )
    return jax.shard_map(
        local,
        mesh=split,
        in_specs=placed,
        out_specs=(P("gz", GX), P("gz"), P(("gz", "gy"), None, GX), P(GX)),
        check_vma=False,
    )
```

```python
import functools
import math

import jax
import jax.numpy as jnp
from jax import lax
from jax.experimental import pallas as pl
from jax.experimental.pallas import tpu as pltpu
from jax.sharding import PartitionSpec as P

NE = 128
NA = 16
G = 8
BLK = 128
GZ = 2
GY = 8
N_GX = 16
GROUP = GZ * GY
BLOCKS = 2 * GROUP
CAP = 4
PAD = 8
f32 = jnp.float32
LOG2E = math.log2(math.e)
HIGH = G // GZ


def rows_at(start):
    return pl.ds(pl.multiple_of(start, 8), 8)


def pair_phase(h, pbuf, jacc, grad):
    zero = jnp.zeros((8, 128), f32)

    def clear(i, _):
        for s in range(8):
            for c in range(3):
                jacc[s, c, rows_at(i * 8), :] = zero
        return 0

    lax.fori_loop(0, 34, clear, 0)

    def itile(tile, carry):
        r0 = pl.multiple_of(tile * 8, 8)
        xi, yi, zi = (pbuf[h, c, pl.ds(r0, 8), :] for c in range(3))

        def one(base, s, acc, keep=None):
            gx, gy, gz, lap, co = acc
            row = base + s
            dx = xi - pbuf[h, 0, pl.ds(row, 8), :]
            dy = yi - pbuf[h, 1, pl.ds(row, 8), :]
            dz = zi - pbuf[h, 2, pl.ds(row, 8), :]
            d2 = (dx * dx + 1.0) + (dy * dy + dz * dz)
            r = lax.rsqrt(d2)
            m = d2 * r + 5.0
            t = lax.rsqrt(m * m)
            c = t * t * r
            b = t * (r + 5.0) + 0.5 * (r * r)
            if keep is not None:
                c = c * keep
                r = r * keep
            cx, cy, cz = c * dx, c * dy, c * dz
            at = rows_at(base + PAD)
            jacc[s, 0, at, :] += cx
            jacc[s, 1, at, :] += cy
            jacc[s, 2, at, :] += cz
            return (gx + cx, gy + cy, gz + cz, lap + c * b, co + r)

        def eight(turn, acc):
            base = pl.multiple_of(r0 + turn * 8, 8)
            for s in range(8):
                acc = one(base, s, acc)
            return acc

        acc = (zero, zero, zero, carry[0], carry[1])
        for s in range(1, 8):
            acc = one(r0, s, acc)
        acc = lax.fori_loop(1, 8, eight, acc)
        keep = jnp.where(tile < 8, f32(1), f32(0))
        acc = one(pl.multiple_of(r0 + 64, 8), 0, acc, keep)
        for c in range(3):
            grad[h, c, pl.ds(r0, 8), :] = acc[c]
        return acc[3], acc[4]

    lap, co = lax.fori_loop(0, 16, itile, (zero, zero))

    def fold(tile, jj):
        r0 = pl.multiple_of(tile * 8, 8)
        for c in range(3):
            g = grad[h, c, pl.ds(r0, 8), :]
            for s in range(8):
                g = g - jacc[s, c, pl.ds(r0 + (PAD - s), 8), :]
                g = g - jacc[s, c, pl.ds(r0 + (PAD - s) + 128, 8), :]
            grad[h, c, pl.ds(r0, 8), :] = g
            jj = jj + g * g
        return jj

    jj = lax.fori_loop(0, 16, fold, zero)
    return 5.0 * co - 125.0 * lap - 78.125 * jj


def orbital_phase(h, g, pbuf, grad, k_ref, esum, lsum, drift, tiles=4):
    zero = jnp.zeros((8, 128), f32)

    def group(q, acc):
        en, lg = acc
        at = [rows_at(q * (8 * tiles) + 8 * i) for i in range(tiles)]
        ph, gx, gy, gz, la, po = ([zero] * tiles for _ in range(6))
        for a in range(NA):
            row = g * NA + a
            cx, cy, cz, na, co, al, a2, ch = (k_ref[i, row] for i in range(8))
            for i in range(tiles):
                vx = pbuf[h, 0, at[i], :] - cx
                vy = pbuf[h, 1, at[i], :] - cy
                vz = pbuf[h, 2, at[i], :] - cz
                d2 = (vx * vx + 1.0) + (vy * vy + vz * vz)
                r = lax.rsqrt(d2)
                d = d2 * r
                e = co * jnp.exp2(na * d)
                w = e * (al * r)
                t2 = r * (r + al) + 2.0
                ph[i] = ph[i] + e
                gx[i] = gx[i] + w * vx
                gy[i] = gy[i] + w * vy
                gz[i] = gz[i] + w * vz
                la[i] = la[i] + (a2 * e - w * t2)
                po[i] = po[i] + ch * r
        for i in range(tiles):
            inv = 1.0 / ph[i]
            jx, jy, jz = (grad[h, c, at[i], :] for c in range(3))
            dot = gx[i] * jx + gy[i] * jy + gz[i] * jz
            en = en + (62.5 * dot - 12.5 * la[i]) * inv - 5.0 * po[i]
            lg = lg + jnp.log(ph[i])
            if drift is not None:
                for c, (og, jg) in enumerate(((gx[i], jx), (gy[i], jy), (gz[i], jz))):
                    p = pbuf[h, c, at[i], :] * 0.2
                    drift[h, q * tiles + i, c] = p + (0.125 * jg - (0.05 * og) * inv)
        return en, lg

    en, lg = lax.fori_loop(0, NE // (8 * tiles), group, (zero, zero))
    esum[h, g] = en
    lsum[h, g] = lg


def step_kernel(
    pos_ref, noise_ref, k_ref, nuc_ref, aw_ref, pick_ref, slot_ref,
    le_ref, est_ref, np_ref, nw_ref,
    posbuf, pbuf, jacc, grad, esum, lsum, erow, lrow, drift, dstage, sendbuf, recvbuf,
    moved, msg, emsg, kept, gmsg, gmsg_in, arrived,
    ps, pr, ds_, dr, es, er, bs, br, ms, mr,
):
    gz = lax.axis_index("gz")
    gx = lax.axis_index("gx")
    gy = lax.axis_index("gy")
    me = gz * GY + gy
    order = sorted(range(1, GROUP), key=lambda u: min(u % GY, GY - u % GY))

    def group_peer(u):
        z = lax.rem(gz + u // GY, GZ)
        y = lax.rem(gy + u % GY, GY)
        return z, y, z * GY + y

    def remote(src, dst, send, recv, peer):
        return pltpu.make_async_remote_copy(
            src_ref=src, dst_ref=dst, send_sem=send, recv_sem=recv,
            device_id=peer, device_id_type=pl.DeviceIdType.MESH,
        )

    barrier = pltpu.get_barrier_semaphore()
    for u in order:
        z, y, _ = group_peer(u)
        pl.semaphore_signal(barrier, inc=1, device_id=(z, gx, y), device_id_type=pl.DeviceIdType.MESH)
    for u in range(1, N_GX):
        pl.semaphore_signal(
            barrier, inc=1, device_id=(gz, lax.rem(gx + u, N_GX), gy), device_id_type=pl.DeviceIdType.MESH
        )
    pl.semaphore_wait(barrier, GROUP + N_GX - 2)

    waits = []
    pos_in = []
    for u in order:
        z, y, rank = group_peer(u)
        for h in range(2):
            cp = remote(
                pos_ref.at[:, :, pl.ds(pl.multiple_of(rank * 256 + h * 128, 128), 128)],
                posbuf.at[h, :, rows_at(me * 8), :],
                ps.at[h, u], pr.at[h, u], (z, gx, y),
            )
            cp.start()
            pos_in.append(cp)
    for h in range(2):
        posbuf[h, :, rows_at(me * 8), :] = pos_ref[
            :, :, pl.ds(pl.multiple_of(me * 256 + h * 128, 128), 128)
        ]
    for cp in pos_in:
        cp.wait_recv()

    def scale(i, _):
        for h in range(2):
            for c in range(3):
                p = posbuf[h, c, rows_at(i * 8), :] * 5.0
                pbuf[h, c, rows_at(i * 8), :] = p
                pbuf[h, c, rows_at(i * 8 + 128), :] = p
        return 0

    lax.fori_loop(0, 16, scale, 0)

    base = []
    drift_in = []
    for h in range(2):
        base.append(pair_phase(h, pbuf, jacc, grad))
        orbital_phase(h, 0, pbuf, grad, k_ref, esum, lsum, drift)
        for u in order:
            z, y, rank = group_peer(u)
            cp = remote(
                drift.at[h, rank], dstage.at[me * 2 + h], ds_.at[h, u], dr.at[h, u], (z, gx, y)
            )
            cp.start()
            drift_in.append(cp)
        for c in range(3):
            dstage[me * 2 + h, c] = drift[h, me, c]

    def geometry(g, _):
        for h in range(2):
            orbital_phase(h, g, pbuf, grad, k_ref, esum, lsum, None)
        return 0

    lax.fori_loop(1, FIRST, geometry, 0)

    for cp in drift_in:
        cp.wait_recv()
    blocks_in = []
    for b in range(BLOCKS):
        for c in range(3):
            moved[b, c] = dstage[b, c] + 0.1 * noise_ref[c, :, b * 128:(b + 1) * 128]

    def pack(q, _):
        for n in range(CAP):
            sendbuf[q * CAP + n] = moved[pick_ref[q * CAP + n]]
        return 0

    lax.fori_loop(0, N_GX, pack, 0)
    for u in range(1, N_GX):
        q = lax.rem(gx + u, N_GX)
        cp = remote(
            sendbuf.at[pl.ds(q * CAP, CAP)], recvbuf.at[pl.ds(gx * CAP, CAP)],
            bs.at[u], br.at[u], (gz, q, gy),
        )
        cp.start()
        blocks_in.append(cp)
    for n in range(CAP):
        for c in range(3):
            recvbuf[gx * CAP + n, c] = sendbuf[gx * CAP + n, c]

    lax.fori_loop(FIRST, G, geometry, 0)

    num = jnp.zeros((G, 128), f32)
    den = jnp.zeros((G, 128), f32)
    for h in range(2):
        extra = jnp.sum(base[h], axis=0, keepdims=True)
        for g in range(G):
            erow[h, g:g + 1, :] = jnp.sum(esum[h, g], axis=0, keepdims=True) + extra
            lrow[h, g:g + 1, :] = jnp.sum(lsum[h, g], axis=0, keepdims=True)
        le = (erow[h] + nuc_ref[...]) * (1.0 / NE)
        logs = lrow[h]
        omega = aw_ref[pl.ds(me * 2 + h, 1), :] * jnp.exp(2.0 * (logs - logs[0:1]))
        num = num + omega * le
        den = den + omega
        for z in range(GZ):
            msg[z, h * HIGH:(h + 1) * HIGH, :] = le[z * HIGH:(z + 1) * HIGH]
            msg[z, 16 + h:17 + h, :] = le[0:1]
    lane = lax.broadcasted_iota(jnp.int32, (G, 128), 1)
    both = jnp.where(
        lane == 0,
        jnp.sum(num, axis=1, keepdims=True),
        jnp.where(lane == 1, jnp.sum(den, axis=1, keepdims=True), 0.0),
    )
    for z in range(GZ):
        msg[z, 8:16, :] = both
    msg_in = []
    for u in order:
        z, y, rank = group_peer(u)
        cp = remote(msg.at[z], emsg.at[me], es.at[u], er.at[u], (z, gx, y))
        cp.start()
        msg_in.append(cp)
    emsg[me] = msg[gz]
    for cp in msg_in:
        cp.wait_recv()
    total = jnp.zeros((G, 128), f32)
    for s in range(GROUP):
        total = total + emsg[s, 8:16, :]
        for h in range(2):
            kept[2 * s + h, 0:1, :] = emsg[s, 16 + h:17 + h, :]
            kept[2 * s + h, 1:2, :] = aw_ref[2 * s + h:2 * s + h + 1, :]

    def packw(q, _):
        for n in range(CAP):
            gmsg[q, 2 * n:2 * n + 2, :] = kept[pick_ref[q * CAP + n]][0:2]
        gmsg[q, 8:16, :] = total
        return 0

    lax.fori_loop(0, N_GX, packw, 0)
    sums_in = []
    for u in range(1, N_GX):
        q = lax.rem(gx + u, N_GX)
        cp = remote(
            gmsg.at[q], gmsg_in.at[pl.ds(pl.multiple_of(gx * 16, 16), 16)],
            ms.at[u], mr.at[u], (gz, q, gy),
        )
        cp.start()
        sums_in.append(cp)
    gmsg_in[pl.ds(pl.multiple_of(gx * 16, 16), 16), :] = gmsg[gx]
    for s in range(GROUP):
        for h in range(2):
            le_ref[:, s * 256 + h * 128:s * 256 + (h + 1) * 128] = emsg[s, h * HIGH:(h + 1) * HIGH, :]
    for cp in blocks_in:
        cp.wait_recv()
    for d in range(BLOCKS):
        block = recvbuf[slot_ref[d]]
        for c in range(3):
            np_ref[c, :, d * 128:(d + 1) * 128] = block[c]
    for cp in sums_in:
        cp.wait_recv()
    whole = jnp.zeros((G, 128), f32)
    for q in range(N_GX):
        whole = whole + gmsg_in[q * 16 + 8:q * 16 + 16, :]
        for n in range(CAP):
            arrived[q * CAP + n, 0:2, :] = gmsg_in[q * 16 + 2 * n:q * 16 + 2 * n + 2, :]
    estimate = whole[:, 0:1] / whole[:, 1:2]
    est_ref[...] = jnp.broadcast_to(
        jnp.where(gz == 0, estimate[0:HIGH], estimate[HIGH:G]), (HIGH, 128)
    )
    first = estimate[0:1, 0:1]
    for d in range(BLOCKS):
        pair = arrived[slot_ref[d]]
        nw_ref[d:d + 1, :] = pair[1:2] * jnp.exp(first - pair[0:1])
    for cp in pos_in + drift_in + blocks_in + msg_in + sums_in:
        cp.wait_send()


FIRST = 4


def nuclear(centers, charges):
    offsets = centers[:, :, None, :] - centers[:, None, :, :]
    identity = jnp.eye(NA, dtype=f32)
    distance = jnp.sqrt(jnp.sum(offsets * offsets, axis=3) + identity)
    pairs = charges[:, None] * charges[None, :] * (1.0 - identity)
    return 0.5 * jnp.sum(pairs / distance, axis=(1, 2))


def tables(branch_source, gx):
    own = branch_source.reshape(N_GX, BLOCKS)
    device = own // BLOCKS
    k = jnp.arange(BLOCKS, dtype=jnp.int32)
    same = (device[:, :, None] == device[:, None, :]) & (k[None, None, :] < k[None, :, None])
    rank = jnp.sum(same.astype(jnp.int32), axis=2)
    hit = (device == gx)[:, None, :] & (rank[:, None, :] == jnp.arange(CAP, dtype=jnp.int32)[None, :, None])
    pick = jnp.sum(jnp.where(hit, own[:, None, :] % BLOCKS, 0), axis=2)
    slot = device * CAP + rank
    return pick.reshape(-1), lax.dynamic_slice_in_dim(slot, gx, 1, 0).reshape(-1)


def local(
    positions, diffusion_noise, base_nuclei, displacements, charges, orbital_decay,
    coefficients, weights, counts, branch_source,
):
    gx = lax.axis_index("gx")
    centers = base_nuclei[None, :, :] + displacements
    decay = orbital_decay * 0.2
    spread = lambda v: jnp.broadcast_to(v[None, :], (G, NA))
    consts = jnp.stack(
        [centers[..., 0] * 5.0, centers[..., 1] * 5.0, centers[..., 2] * 5.0,
         spread(decay * -LOG2E), spread(coefficients), spread(decay), spread(decay * decay), spread(charges)]
    ).reshape(8, G * NA)
    nuc = jnp.broadcast_to(nuclear(centers, charges)[:, None], (G, 128))
    alive = (jnp.arange(BLK, dtype=jnp.int32)[None, :] < counts[:, None]).astype(f32)
    aw = weights.reshape(BLOCKS, BLK) * alive
    pick, slot = tables(branch_source, gx)
    vmem = pl.BlockSpec(memory_space=pltpu.VMEM)
    smem = pl.BlockSpec(memory_space=pltpu.SMEM)
    dma = pltpu.SemaphoreType.DMA
    v = lambda *shape: pltpu.VMEM(shape, f32)
    le, est, new_pos, new_w = pl.pallas_call(
        step_kernel,
        out_shape=(
            jax.ShapeDtypeStruct((HIGH, GROUP * 256), f32),
            jax.ShapeDtypeStruct((HIGH, 128), f32),
            jax.ShapeDtypeStruct((3, 8, GROUP * 256), f32),
            jax.ShapeDtypeStruct((BLOCKS, BLK), f32),
        ),
        in_specs=[vmem, vmem, smem, vmem, vmem, smem, smem],
        out_specs=(vmem,) * 4,
        scratch_shapes=[
            v(2, 3, 128, 128), v(2, 3, 256, 128), v(8, 3, 34 * 8, 128), v(2, 3, 128, 128),
            v(2, G, 8, 128), v(2, G, 8, 128), v(2, G, 128), v(2, G, 128),
            v(2, GROUP, 3, 8, 128), v(BLOCKS, 3, 8, 128), v(N_GX * CAP, 3, 8, 128), v(N_GX * CAP, 3, 8, 128),
            v(BLOCKS, 3, 8, 128), v(GZ, 24, 128), v(GROUP, 24, 128), v(BLOCKS, 8, 128), v(N_GX, 16, 128),
            v(N_GX * 16, 128), v(N_GX * CAP, 8, 128),
            dma((2, GROUP)), dma((2, GROUP)), dma((2, GROUP)), dma((2, GROUP)),
            dma((GROUP,)), dma((GROUP,)), dma((N_GX,)), dma((N_GX,)), dma((N_GX,)), dma((N_GX,)),
        ],
        compiler_params=pltpu.CompilerParams(
            collective_id=0, has_side_effects=True, vmem_limit_bytes=40 * 2**20
        ),
    )(
        positions.transpose(1, 0, 2), diffusion_noise.transpose(1, 0, 2), consts, nuc, aw, pick, slot
    )
    return le, est[:, 0], new_pos.transpose(1, 0, 2), new_w.reshape(-1)


def solution(mesh):
    placed = (
        P(("gz", "gy"), None, "gx"), P(("gz", "gy"), None, "gx"), P(), P(), P(), P(), P(),
        P("gx"), P("gx"), P(),
    )
    return jax.shard_map(
        local,
        mesh=mesh,
        in_specs=placed,
        out_specs=(P("gz", "gx"), P("gz"), P(("gz", "gy"), None, "gx"), P("gx")),
        check_vma=False,
    )
```

```python
import functools
import math

import jax
import jax.numpy as jnp
from jax import lax
from jax.experimental import pallas as pl
from jax.experimental.pallas import tpu as pltpu
from jax.sharding import PartitionSpec as P

NE = 128
NA = 16
G = 8
BLK = 128
GZ = 2
GY = 8
N_GX = 16
GROUP = GZ * GY
BLOCKS = 2 * GROUP
CAP = 4
PAD = 8
f32 = jnp.float32
i32 = jnp.int32
TILES = NE // 8
EARLY = 4
MIDDLE = 4
LOG2E = math.log2(math.e)
HIGH = G // GZ


def rows_at(start):
    return pl.ds(pl.multiple_of(start, 8), 8)


def constants(base_ref, disp_ref, charge_ref, decay_ref, coef_ref, cc, kc):
    def per_atom(a, _):
        for c in range(3):
            for g in range(G):
                cc[g, a, c] = jnp.full((8, 128), (base_ref[a, c] + disp_ref[g, a, c]) * 5.0, f32)
        al = decay_ref[a] * 0.2
        for i, s in enumerate((al * -LOG2E, coef_ref[a], al, al * al, charge_ref[a])):
            kc[a, i] = jnp.full((8, 128), s, f32)
        return 0

    lax.fori_loop(0, NA, per_atom, 0)


def repulsion(cc, kc, nuc):
    sub = lax.broadcasted_iota(jnp.int32, (8, 128), 0)

    def gather(a, _):
        for c in range(3):
            value = cc[0, a, c]
            for g in range(1, G):
                value = jnp.where(sub == g, cc[g, a, c], value)
            nuc[a, c] = value
        return 0

    lax.fori_loop(0, NA, gather, 0)

    def repel(a, total):
        for b in range(1, NA):
            far = b > a
            dx, dy, dz = (nuc[a, c] - nuc[b, c] for c in range(3))
            q = kc[a, 4] * kc[b, 4] * jnp.where(far, f32(1), f32(0))
            d2 = dx * dx + dy * dy + dz * dz + jnp.where(far, f32(0), f32(1))
            total = total + q * lax.rsqrt(d2)
        return total

    return 5.0 * lax.fori_loop(0, NA - 1, repel, jnp.zeros((8, 128), f32))


def take_tile(tile, posbuf, pbuf):
    for h in range(2):
        for c in range(3):
            p = posbuf[h, c, rows_at(tile * 8), :] * 5.0
            pbuf[h, c, rows_at(tile * 8), :] = p
            pbuf[h, c, rows_at(tile * 8 + 128), :] = p


def orbital_tiles(ranks, g, pbuf, cc, kc, og, esum, lsum):
    zero = jnp.zeros((8, 128), f32)
    at = [(h, rank) for rank in ranks for h in range(2)]
    acc = [[zero] * 6 for _ in at]
    for a in range(NA):
        cx, cy, cz = (cc[g, a, c] for c in range(3))
        na, co, al, a2, ch = (kc[a, i] for i in range(5))
        for i, (h, rank) in enumerate(at):
            ph, gx, gy, gz, la, po = acc[i]
            vx = pbuf[h, 0, rows_at(rank * 8), :] - cx
            vy = pbuf[h, 1, rows_at(rank * 8), :] - cy
            vz = pbuf[h, 2, rows_at(rank * 8), :] - cz
            d2 = (vx * vx + 1.0) + (vy * vy + vz * vz)
            r = lax.rsqrt(d2)
            ex = co * jnp.exp2(na * (d2 * r))
            w = ex * (al * r)
            t2 = r * (r + al) + 2.0
            acc[i] = [ph + ex, gx + w * vx, gy + w * vy, gz + w * vz, la + (a2 * ex - w * t2), po + ch * r]
    for i, (h, rank) in enumerate(at):
        ph, gx, gy, gz, la, po = acc[i]
        inv = 1.0 / ph
        for c, m in enumerate((gx, gy, gz)):
            og[g, h, c, rows_at(rank * 8), :] = m * inv
        esum[g, h] += -12.5 * (la * inv) - 5.0 * po
        lsum[g, h] += jnp.log(ph)


def pair_phase(h, pbuf, jacc, grad):
    zero = jnp.zeros((8, 128), f32)

    def clear(i, _):
        for s in range(8):
            for c in range(3):
                jacc[s, c, rows_at(i * 8), :] = zero
        return 0

    lax.fori_loop(0, 27, clear, 0)

    def itile(tile, carry):
        r0 = pl.multiple_of(tile * 8, 8)
        xi, yi, zi = (pbuf[h, c, pl.ds(r0, 8), :] for c in range(3))

        def one(m, s, acc, keep=None):
            gx, gy, gz, lap, co = acc
            row = r0 + (m * 8 + s)
            dx = xi - pbuf[h, 0, pl.ds(row, 8), :]
            dy = yi - pbuf[h, 1, pl.ds(row, 8), :]
            dz = zi - pbuf[h, 2, pl.ds(row, 8), :]
            d2 = (dx * dx + 1.0) + (dy * dy + dz * dz)
            r = lax.rsqrt(d2)
            q = d2 * r + 5.0
            t = lax.rsqrt(q * q)
            c = t * t * r
            b = t * (r + 5.0) + 0.5 * (r * r)
            if keep is not None:
                c = c * keep
                r = r * keep
            cx, cy, cz = c * dx, c * dy, c * dz
            at = rows_at(r0 + (m * 8 + PAD))
            jacc[s, 0, at, :] += cx
            jacc[s, 1, at, :] += cy
            jacc[s, 2, at, :] += cz
            return (gx + cx, gy + cy, gz + cz, lap + c * b, co + r)

        acc = (zero, zero, zero, carry[0], carry[1])
        for k in range(1, 64):
            acc = one(k // 8, k % 8, acc)
        keep = jnp.where(tile < 8, f32(1), f32(0))
        acc = one(8, 0, acc, keep)
        for c in range(3):
            grad[h, c, pl.ds(r0, 8), :] = acc[c]
        return acc[3], acc[4]

    lap, co = lax.fori_loop(0, TILES, itile, (zero, zero))

    def fold(tile, jj, wrap):
        r0 = pl.multiple_of(tile * 8, 8)
        for c in range(3):
            g = grad[h, c, pl.ds(r0, 8), :]
            for s in range(8):
                g = g - jacc[s, c, pl.ds(r0 + (PAD - s), 8), :]
                if wrap:
                    g = g - jacc[s, c, pl.ds(r0 + (PAD - s) + 128, 8), :]
            grad[h, c, pl.ds(r0, 8), :] = g
            jj = jj + g * g
        return jj

    jj = lax.fori_loop(0, 9, lambda i, j: fold(i, j, True), zero)
    jj = lax.fori_loop(9, TILES, lambda i, j: fold(i, j, False), jj)
    return jnp.sum(5.0 * co - 125.0 * lap - 78.125 * jj, axis=0, keepdims=True)


def cross(g, grad, og, esum):
    for h in range(2):
        acc = jnp.zeros((8, 128), f32)
        for t in range(TILES):
            dot = og[g, h, 0, rows_at(t * 8), :] * grad[h, 0, rows_at(t * 8), :]
            for c in (1, 2):
                dot = dot + og[g, h, c, rows_at(t * 8), :] * grad[h, c, rows_at(t * 8), :]
            acc = acc + dot
        esum[g, h] += 62.5 * acc


def drift_half(h, pbuf, grad, og, out):
    def one(t, _):
        for c in range(3):
            out[h, t, c] = 0.2 * pbuf[h, c, rows_at(t * 8), :] + (
                0.125 * grad[h, c, rows_at(t * 8), :] - 0.05 * og[0, h, c, rows_at(t * 8), :]
            )
        return 0

    lax.fori_loop(0, TILES, one, 0)


def exchange_tables(gx, source_ref, vtable):
    source = source_ref[...]
    device = source // BLOCKS
    lane = lax.broadcasted_iota(i32, (4, 128), 1) % BLOCKS
    rank = jnp.zeros((4, 128), i32)
    for j in range(1, BLOCKS):
        same = (pltpu.roll(device, j, 1) == device) & (lane >= j)
        rank = rank + jnp.where(same, 1, 0)
    vtable[0:4, :] = device * CAP + rank
    for n in range(CAP):
        pick = jnp.where((device == gx) & (rank == n), source % BLOCKS, 0)
        for j in (1, 2, 4, 8, 16):
            pick = pick + pltpu.roll(pick, j, 1)
        vtable[4 + 4 * n:8 + 4 * n, :] = pick


def step_kernel(
    pos_ref, noise_ref, base_ref, disp_ref, charge_ref, decay_ref, coef_ref, w_ref, count_ref, source_ref,
    le_ref, est_ref, np_ref, nw_ref,
    posbuf, pbuf, jacc, grad, cc, kc, nuc, og, esum, lsum, erow, lrow, drift, dstage, sendbuf, recvbuf,
    moved, msg, emsg, kept, gmsg, gmsg_in, arrived, aw_ref, vtable, table, ts,
    ps, pr, ds_, dr, es, er, bs, br, ms, mr,
):
    gz = lax.axis_index("gz")
    gx = lax.axis_index("gx")
    gy = lax.axis_index("gy")
    me = gz * GY + gy
    order = sorted(range(1, GROUP), key=lambda u: min(u % GY, GY - u % GY))

    def group_peer(u):
        z = lax.rem(gz + u // GY, GZ)
        y = lax.rem(gy + u % GY, GY)
        return z, y, z * GY + y

    def source_rank(u):
        z = lax.rem(gz + GZ - u // GY, GZ)
        return z * GY + lax.rem(gy + GY - u % GY, GY)

    def remote(src, dst, send, recv, peer):
        return pltpu.make_async_remote_copy(
            src_ref=src, dst_ref=dst, send_sem=send, recv_sem=recv,
            device_id=peer, device_id_type=pl.DeviceIdType.MESH,
        )

    barrier = pltpu.get_barrier_semaphore()
    for u in order:
        z, y, _ = group_peer(u)
        pl.semaphore_signal(barrier, inc=1, device_id=(z, gx, y), device_id_type=pl.DeviceIdType.MESH)
    for u in range(1, N_GX):
        pl.semaphore_signal(
            barrier, inc=1, device_id=(gz, lax.rem(gx + u, N_GX), gy), device_id_type=pl.DeviceIdType.MESH
        )
    constants(base_ref, disp_ref, charge_ref, decay_ref, coef_ref, cc, kc)
    for h in range(2):
        posbuf[h, :, rows_at(me * 8), :] = pos_ref[
            :, :, pl.ds(pl.multiple_of(me * 256 + h * 128, 128), 128)
        ]
    esum[...] = jnp.zeros_like(esum)
    lsum[...] = jnp.zeros_like(lsum)
    take_tile(me, posbuf, pbuf)
    exchange_tables(gx, source_ref, vtable)
    to_smem = pltpu.make_async_copy(vtable, table, ts)
    to_smem.start()
    lane_row = lax.broadcasted_iota(i32, (1, 128), 1)
    for b in range(BLOCKS):
        alive = jnp.where(lane_row < count_ref[b], 1.0, 0.0)
        aw_ref[b:b + 1, :] = w_ref[b:b + 1, :] * alive
    pl.semaphore_wait(barrier, GROUP + N_GX - 2)

    pos_in = {}
    for u in order:
        z, y, rank = group_peer(u)
        for h in range(2):
            cp = remote(
                pos_ref.at[:, :, pl.ds(pl.multiple_of(rank * 256 + h * 128, 128), 128)],
                posbuf.at[h, :, rows_at(me * 8), :],
                ps.at[h, u], pr.at[h, u], (z, gx, y),
            )
            cp.start()
            pos_in[u, h] = cp

    def arrive(u):
        for h in range(2):
            pos_in[u, h].wait_recv()
        take_tile(source_rank(u), posbuf, pbuf)

    def geometries(u, first, last):
        def one(g, _):
            orbital_tiles([source_rank(u)], g, pbuf, cc, kc, og, esum, lsum)
            return 0

        lax.fori_loop(first, last, one, 0)

    every = [0] + order
    geometries(0, 0, G)
    for u in every[1:2 * EARLY]:
        arrive(u)
        geometries(u, 0, G)
    for u in every[2 * EARLY:]:
        arrive(u)
        geometries(u, 0, 1)

    base = []
    drift_in = []
    for h in range(2):
        base.append(pair_phase(h, pbuf, jacc, grad))
        drift_half(h, pbuf, grad, og, drift)
        for u in order:
            z, y, rank = group_peer(u)
            cp = remote(
                drift.at[h, rank], dstage.at[me * 2 + h], ds_.at[h, u], dr.at[h, u], (z, gx, y)
            )
            cp.start()
            drift_in.append(cp)
        for c in range(3):
            dstage[me * 2 + h, c] = drift[h, me, c]

    late = every[2 * EARLY:]
    for u in late[:MIDDLE]:
        geometries(u, 1, G)

    for cp in drift_in:
        cp.wait_recv()
    blocks_in = []
    for b in range(BLOCKS):
        for c in range(3):
            moved[b, c] = dstage[b, c] + 0.1 * noise_ref[c, :, b * 128:(b + 1) * 128]

    def pack(q, _):
        for n in range(CAP):
            sendbuf[q * CAP + n] = moved[table[4 + 4 * n + q // 4, lax.rem(q, 4) * 32 + 31]]
        return 0

    to_smem.wait()
    lax.fori_loop(0, N_GX, pack, 0)
    for u in range(1, N_GX):
        q = lax.rem(gx + u, N_GX)
        cp = remote(
            sendbuf.at[pl.ds(q * CAP, CAP)], recvbuf.at[pl.ds(gx * CAP, CAP)],
            bs.at[u], br.at[u], (gz, q, gy),
        )
        cp.start()
        blocks_in.append(cp)
    for n in range(CAP):
        for c in range(3):
            recvbuf[gx * CAP + n, c] = sendbuf[gx * CAP + n, c]

    for u in late[MIDDLE:]:
        geometries(u, 1, G)
    lax.fori_loop(0, G, lambda g, _: (cross(g, grad, og, esum), 0)[1], 0)
    nuclear = repulsion(cc, kc, nuc)

    num = jnp.zeros((G, 128), f32)
    den = jnp.zeros((G, 128), f32)
    for h in range(2):
        for g in range(G):
            erow[h, g:g + 1, :] = jnp.sum(esum[g, h], axis=0, keepdims=True) + base[h]
            lrow[h, g:g + 1, :] = jnp.sum(lsum[g, h], axis=0, keepdims=True)
        le = (erow[h] + nuclear) * (1.0 / NE)
        logs = lrow[h]
        omega = aw_ref[pl.ds(me * 2 + h, 1), :] * jnp.exp(2.0 * (logs - logs[0:1]))
        num = num + omega * le
        den = den + omega
        for z in range(GZ):
            msg[z, h * HIGH:(h + 1) * HIGH, :] = le[z * HIGH:(z + 1) * HIGH]
            msg[z, 16 + h:17 + h, :] = le[0:1]
    lane = lax.broadcasted_iota(jnp.int32, (G, 128), 1)
    both = jnp.where(
        lane == 0,
        jnp.sum(num, axis=1, keepdims=True),
        jnp.where(lane == 1, jnp.sum(den, axis=1, keepdims=True), 0.0),
    )
    for z in range(GZ):
        msg[z, 8:16, :] = both
    msg_in = []
    for u in order:
        z, y, rank = group_peer(u)
        cp = remote(msg.at[z], emsg.at[me], es.at[u], er.at[u], (z, gx, y))
        cp.start()
        msg_in.append(cp)
    emsg[me] = msg[gz]
    for cp in msg_in:
        cp.wait_recv()
    total = jnp.zeros((G, 128), f32)
    for s in range(GROUP):
        total = total + emsg[s, 8:16, :]
        for h in range(2):
            kept[2 * s + h, 0:1, :] = emsg[s, 16 + h:17 + h, :]
            kept[2 * s + h, 1:2, :] = aw_ref[2 * s + h:2 * s + h + 1, :]

    def packw(q, _):
        for n in range(CAP):
            gmsg[q, 2 * n:2 * n + 2, :] = kept[table[4 + 4 * n + q // 4, lax.rem(q, 4) * 32 + 31]][0:2]
        gmsg[q, 8:16, :] = total
        return 0

    lax.fori_loop(0, N_GX, packw, 0)
    sums_in = []
    for u in range(1, N_GX):
        q = lax.rem(gx + u, N_GX)
        cp = remote(
            gmsg.at[q], gmsg_in.at[pl.ds(pl.multiple_of(gx * 16, 16), 16)],
            ms.at[u], mr.at[u], (gz, q, gy),
        )
        cp.start()
        sums_in.append(cp)
    gmsg_in[pl.ds(pl.multiple_of(gx * 16, 16), 16), :] = gmsg[gx]
    for s in range(GROUP):
        for h in range(2):
            le_ref[:, s * 256 + h * 128:s * 256 + (h + 1) * 128] = emsg[s, h * HIGH:(h + 1) * HIGH, :]
    for cp in blocks_in:
        cp.wait_recv()
    for d in range(BLOCKS):
        block = recvbuf[table[gx // 4, lax.rem(gx, 4) * 32 + d]]
        for c in range(3):
            np_ref[c, :, d * 128:(d + 1) * 128] = block[c]
    for cp in sums_in:
        cp.wait_recv()
    whole = jnp.zeros((G, 128), f32)
    for q in range(N_GX):
        whole = whole + gmsg_in[q * 16 + 8:q * 16 + 16, :]
        for n in range(CAP):
            arrived[q * CAP + n, 0:2, :] = gmsg_in[q * 16 + 2 * n:q * 16 + 2 * n + 2, :]
    estimate = whole[:, 0:1] / whole[:, 1:2]
    est_ref[...] = jnp.broadcast_to(
        jnp.where(gz == 0, estimate[0:HIGH], estimate[HIGH:G]), (HIGH, 128)
    )
    first = estimate[0:1, 0:1]
    for d in range(BLOCKS):
        pair = arrived[table[gx // 4, lax.rem(gx, 4) * 32 + d]]
        nw_ref[d:d + 1, :] = pair[1:2] * jnp.exp(first - pair[0:1])
    for cp in list(pos_in.values()) + drift_in + blocks_in + msg_in + sums_in:
        cp.wait_send()


def local(
    positions, diffusion_noise, base_nuclei, displacements, charges, orbital_decay,
    coefficients, weights, counts, branch_source,
):
    vmem = pl.BlockSpec(memory_space=pltpu.VMEM)
    smem = pl.BlockSpec(memory_space=pltpu.SMEM)
    dma = pltpu.SemaphoreType.DMA
    v = lambda *shape: pltpu.VMEM(shape, f32)
    le, est, new_pos, new_w = pl.pallas_call(
        step_kernel,
        out_shape=(
            jax.ShapeDtypeStruct((HIGH, GROUP * 256), f32),
            jax.ShapeDtypeStruct((HIGH, 128), f32),
            jax.ShapeDtypeStruct((3, 8, GROUP * 256), f32),
            jax.ShapeDtypeStruct((BLOCKS, BLK), f32),
        ),
        in_specs=[vmem, vmem, smem, smem, smem, smem, smem, vmem, smem, vmem],
        out_specs=(vmem,) * 4,
        scratch_shapes=[
            v(2, 3, 128, 128), v(2, 3, 256, 128), v(8, 3, 27 * 8, 128), v(2, 3, 128, 128),
            v(G, NA, 3, 8, 128), v(NA, 5, 8, 128), v(NA, 3, 8, 128), v(G, 2, 3, 128, 128),
            v(G, 2, 8, 128), v(G, 2, 8, 128), v(2, G, 128), v(2, G, 128),
            v(2, GROUP, 3, 8, 128), v(BLOCKS, 3, 8, 128), v(N_GX * CAP, 3, 8, 128), v(N_GX * CAP, 3, 8, 128),
            v(BLOCKS, 3, 8, 128), v(GZ, 24, 128), v(GROUP, 24, 128), v(BLOCKS, 8, 128), v(N_GX, 16, 128),
            v(N_GX * 16, 128), v(N_GX * CAP, 8, 128), v(BLOCKS, BLK),
            pltpu.VMEM((24, 128), i32), pltpu.SMEM((24, 128), i32), pltpu.SemaphoreType.DMA,
            dma((2, GROUP)), dma((2, GROUP)), dma((2, GROUP)), dma((2, GROUP)),
            dma((GROUP,)), dma((GROUP,)), dma((N_GX,)), dma((N_GX,)), dma((N_GX,)), dma((N_GX,)),
        ],
        compiler_params=pltpu.CompilerParams(
            collective_id=0, has_side_effects=True, vmem_limit_bytes=40 * 2**20
        ),
    )(
        positions.transpose(1, 0, 2), diffusion_noise.transpose(1, 0, 2), base_nuclei, displacements,
        charges, orbital_decay, coefficients, weights.reshape(BLOCKS, BLK), counts,
        branch_source.reshape(4, 128),
    )
    return le, est[:, 0], new_pos.transpose(1, 0, 2), new_w.reshape(-1)


def solution(mesh):
    placed = (
        P(("gz", "gy"), None, "gx"), P(("gz", "gy"), None, "gx"), P(), P(), P(), P(), P(),
        P("gx"), P("gx"), P(),
    )
    return jax.shard_map(
        local,
        mesh=mesh,
        in_specs=placed,
        out_specs=(P("gz", "gx"), P("gz"), P(("gz", "gy"), None, "gx"), P("gx")),
        check_vma=False,
    )
```

```python
import functools
import math

import jax
import jax.numpy as jnp
from jax import lax
from jax.experimental import pallas as pl
from jax.experimental.pallas import tpu as pltpu
from jax.sharding import PartitionSpec as P

NE = 128
NA = 16
G = 8
BLK = 128
GZ = 2
GY = 8
N_GX = 16
GROUP = GZ * GY
BLOCKS = 2 * GROUP
CAP = 4
PAD = 8
f32 = jnp.float32
i32 = jnp.int32
TILES = NE // 8
MIDDLE = 8
LOG2E = math.log2(math.e)
HIGH = G // GZ


def rows_at(start):
    return pl.ds(pl.multiple_of(start, 8), 8)


def constants(base_ref, disp_ref, charge_ref, decay_ref, coef_ref, cc, kc):
    def per_atom(a, _):
        for c in range(3):
            for g in range(G):
                cc[g, a, c] = jnp.full((8, 128), (base_ref[c, a] + disp_ref[c, g, a]) * 5.0, f32)
        al = decay_ref[a] * 0.2
        for i, s in enumerate((al * -LOG2E, coef_ref[a], al, al * al, charge_ref[a])):
            kc[a, i] = jnp.full((8, 128), s, f32)
        return 0

    lax.fori_loop(0, NA, per_atom, 0)


def repulsion(cc, kc, nuc):
    sub = lax.broadcasted_iota(jnp.int32, (8, 128), 0)

    def gather(a, _):
        for c in range(3):
            value = cc[0, a, c]
            for g in range(1, G):
                value = jnp.where(sub == g, cc[g, a, c], value)
            nuc[a, c] = value
        return 0

    lax.fori_loop(0, NA, gather, 0)

    def repel(a, total):
        for b in range(1, NA):
            far = b > a
            dx, dy, dz = (nuc[a, c] - nuc[b, c] for c in range(3))
            q = kc[a, 4] * kc[b, 4] * jnp.where(far, f32(1), f32(0))
            d2 = dx * dx + dy * dy + dz * dz + jnp.where(far, f32(0), f32(1))
            total = total + q * lax.rsqrt(d2)
        return total

    return 5.0 * lax.fori_loop(0, NA - 1, repel, jnp.zeros((8, 128), f32))


def take_tile(h, tile, posbuf, pbuf):
    for c in range(3):
        p = posbuf[h, c, rows_at(tile * 8), :] * 5.0
        pbuf[h, c, rows_at(tile * 8), :] = p
        pbuf[h, c, rows_at(tile * 8 + 128), :] = p


def orbital_tiles(at, g, pbuf, cc, kc, og, esum, lsum):
    zero = jnp.zeros((8, 128), f32)
    acc = [[zero] * 6 for _ in at]
    for a in range(NA):
        cx, cy, cz = (cc[g, a, c] for c in range(3))
        na, co, al, a2, ch = (kc[a, i] for i in range(5))
        for i, (h, rank) in enumerate(at):
            ph, gx, gy, gz, la, po = acc[i]
            vx = pbuf[h, 0, rows_at(rank * 8), :] - cx
            vy = pbuf[h, 1, rows_at(rank * 8), :] - cy
            vz = pbuf[h, 2, rows_at(rank * 8), :] - cz
            d2 = (vx * vx + 1.0) + (vy * vy + vz * vz)
            r = lax.rsqrt(d2)
            ex = co * jnp.exp2(na * (d2 * r))
            w = ex * (al * r)
            t2 = r * (r + al) + 2.0
            acc[i] = [ph + ex, gx + w * vx, gy + w * vy, gz + w * vz, la + (a2 * ex - w * t2), po + ch * r]
    for i, (h, rank) in enumerate(at):
        ph, gx, gy, gz, la, po = acc[i]
        inv = 1.0 / ph
        for c, m in enumerate((gx, gy, gz)):
            og[g, h, c, rows_at(rank * 8), :] = m * inv
        esum[g, h] += -12.5 * (la * inv) - 5.0 * po
        lsum[g, h] += jnp.log(ph)


def pair_phase(h, pbuf, jacc, grad):
    zero = jnp.zeros((8, 128), f32)

    def clear(i, _):
        for s in range(8):
            for c in range(3):
                jacc[s, c, rows_at(i * 8), :] = zero
        return 0

    lax.fori_loop(0, 27, clear, 0)

    def itile(tile, carry):
        r0 = pl.multiple_of(tile * 8, 8)
        xi, yi, zi = (pbuf[h, c, pl.ds(r0, 8), :] for c in range(3))

        def one(m, s, acc, keep=None):
            gx, gy, gz, lap, co = acc
            row = r0 + (m * 8 + s)
            dx = xi - pbuf[h, 0, pl.ds(row, 8), :]
            dy = yi - pbuf[h, 1, pl.ds(row, 8), :]
            dz = zi - pbuf[h, 2, pl.ds(row, 8), :]
            d2 = (dx * dx + 1.0) + (dy * dy + dz * dz)
            r = lax.rsqrt(d2)
            q = d2 * r + 5.0
            t = lax.rsqrt(q * q)
            c = t * t * r
            b = t * (r + 5.0) + 0.5 * (r * r)
            if keep is not None:
                c = c * keep
                r = r * keep
            cx, cy, cz = c * dx, c * dy, c * dz
            at = rows_at(r0 + (m * 8 + PAD))
            jacc[s, 0, at, :] += cx
            jacc[s, 1, at, :] += cy
            jacc[s, 2, at, :] += cz
            return (gx + cx, gy + cy, gz + cz, lap + c * b, co + r)

        acc = (zero, zero, zero, carry[0], carry[1])
        for k in range(1, 64):
            acc = one(k // 8, k % 8, acc)
        keep = jnp.where(tile < 8, f32(1), f32(0))
        acc = one(8, 0, acc, keep)
        for c in range(3):
            grad[h, c, pl.ds(r0, 8), :] = acc[c]
        return acc[3], acc[4]

    lap, co = lax.fori_loop(0, TILES, itile, (zero, zero))

    def fold(tile, jj, wrap):
        r0 = pl.multiple_of(tile * 8, 8)
        for c in range(3):
            g = grad[h, c, pl.ds(r0, 8), :]
            for s in range(8):
                g = g - jacc[s, c, pl.ds(r0 + (PAD - s), 8), :]
                if wrap:
                    g = g - jacc[s, c, pl.ds(r0 + (PAD - s) + 128, 8), :]
            grad[h, c, pl.ds(r0, 8), :] = g
            jj = jj + g * g
        return jj

    jj = lax.fori_loop(0, 9, lambda i, j: fold(i, j, True), zero)
    jj = lax.fori_loop(9, TILES, lambda i, j: fold(i, j, False), jj)
    return jnp.sum(5.0 * co - 125.0 * lap - 78.125 * jj, axis=0, keepdims=True)


def cross(g, grad, og, esum):
    for h in range(2):
        acc = jnp.zeros((8, 128), f32)
        for t in range(TILES):
            dot = og[g, h, 0, rows_at(t * 8), :] * grad[h, 0, rows_at(t * 8), :]
            for c in (1, 2):
                dot = dot + og[g, h, c, rows_at(t * 8), :] * grad[h, c, rows_at(t * 8), :]
            acc = acc + dot
        esum[g, h] += 62.5 * acc


def drift_half(h, pbuf, grad, og, out):
    def one(t, _):
        for c in range(3):
            out[h, t, c] = 0.2 * pbuf[h, c, rows_at(t * 8), :] + (
                0.125 * grad[h, c, rows_at(t * 8), :] - 0.05 * og[0, h, c, rows_at(t * 8), :]
            )
        return 0

    lax.fori_loop(0, TILES, one, 0)


def exchange_tables(gx, source_ref, vtable):
    source = source_ref[...]
    device = source // BLOCKS
    lane = lax.broadcasted_iota(i32, (4, 128), 1) % BLOCKS
    rank = jnp.zeros((4, 128), i32)
    for j in range(1, BLOCKS):
        same = (pltpu.roll(device, j, 1) == device) & (lane >= j)
        rank = rank + jnp.where(same, 1, 0)
    vtable[0:4, :] = device * CAP + rank
    for n in range(CAP):
        pick = jnp.where((device == gx) & (rank == n), source % BLOCKS, 0)
        for j in (1, 2, 4, 8, 16):
            pick = pick + pltpu.roll(pick, j, 1)
        vtable[4 + 4 * n:8 + 4 * n, :] = pick


def step_kernel(
    pos_hbm, noise_hbm, base_ref, disp_ref, charge_ref, decay_ref, coef_ref, w_ref, count_ref, source_ref,
    le_ref, est_ref, np_ref, nw_ref,
    pos_ref, noise_ref, posbuf, pbuf, jacc, grad, cc, kc, nuc, og, esum, lsum, erow, lrow, drift, dstage,
    sendbuf, recvbuf, moved, e0out, e0in, kept, arrived, wout, win, sumrow, sums_in, erows, erows_in, allrow, all_in,
    aw_ref, vtable, table, ts, tp, tn,
    ps, pr, ds_, dr, e0s, e0r, bs, br, ws, wr, ss, sr, es, er, gs, gr,
):
    gz = lax.axis_index("gz")
    gx = lax.axis_index("gx")
    gy = lax.axis_index("gy")
    me = gz * GY + gy
    rings = sorted(range(GY), key=lambda u: min(u, GY - u))
    order = [u for dz in rings for u in (GY + dz, dz) if u]

    def group_peer(u):
        z = lax.rem(gz + u // GY, GZ)
        y = lax.rem(gy + u % GY, GY)
        return z, y, z * GY + y

    def source_rank(u):
        z = lax.rem(gz + GZ - u // GY, GZ)
        return z * GY + lax.rem(gy + GY - u % GY, GY)

    def remote(src, dst, send, recv, peer):
        cp = pltpu.make_async_remote_copy(
            src_ref=src, dst_ref=dst, send_sem=send, recv_sem=recv,
            device_id=peer, device_id_type=pl.DeviceIdType.MESH,
        )
        cp.start()
        sent.append(cp)
        return cp

    sent = []
    pos_copy = pltpu.make_async_copy(pos_hbm, pos_ref, tp)
    pos_copy.start()
    noise_copy = pltpu.make_async_copy(noise_hbm, noise_ref, tn)
    noise_copy.start()
    barrier = pltpu.get_barrier_semaphore()
    for u in order:
        z, y, _ = group_peer(u)
        pl.semaphore_signal(barrier, inc=1, device_id=(z, gx, y), device_id_type=pl.DeviceIdType.MESH)
    for u in range(1, N_GX):
        pl.semaphore_signal(
            barrier, inc=1, device_id=(gz, lax.rem(gx + u, N_GX), gy), device_id_type=pl.DeviceIdType.MESH
        )
    constants(base_ref, disp_ref, charge_ref, decay_ref, coef_ref, cc, kc)
    esum[...] = jnp.zeros_like(esum)
    lsum[...] = jnp.zeros_like(lsum)
    exchange_tables(gx, source_ref, vtable)
    to_smem = pltpu.make_async_copy(vtable, table, ts)
    to_smem.start()
    lane_row = lax.broadcasted_iota(i32, (1, 128), 1)
    for b in range(BLOCKS):
        alive = jnp.where(lane_row < count_ref[b], 1.0, 0.0)
        aw_ref[b:b + 1, :] = w_ref[b:b + 1, :] * alive
    pos_copy.wait()
    for h in range(2):
        posbuf[h, :, rows_at(me * 8), :] = pos_ref[
            :, :, pl.ds(pl.multiple_of(me * 256 + h * 128, 128), 128)
        ]
        take_tile(h, me, posbuf, pbuf)
    nuclear = repulsion(cc, kc, nuc)
    pl.semaphore_wait(barrier, GROUP + N_GX - 2)

    pos_in = {}
    for h in range(2):
        for u in order:
            z, y, rank = group_peer(u)
            pos_in[u, h] = remote(
                pos_ref.at[:, :, pl.ds(pl.multiple_of(rank * 256 + h * 128, 128), 128)],
                posbuf.at[h, :, rows_at(me * 8), :],
                ps.at[h, u], pr.at[h, u], (z, gx, y),
            )

    def arrive(h, dz):
        for u in (GY + dz, dz):
            if u:
                pos_in[u, h].wait_recv()
                take_tile(h, source_rank(u), posbuf, pbuf)

    def geometries(h, dz, first, last):
        at = [(h, source_rank(GY + dz)), (h, source_rank(dz))]

        def one(g, _):
            orbital_tiles(at, g, pbuf, cc, kc, og, esum, lsum)
            return 0

        lax.fori_loop(first, last, one, 0)

    base = []
    drift_in = []

    def pairs(h):
        base.append(pair_phase(h, pbuf, jacc, grad))
        drift_half(h, pbuf, grad, og, drift)
        for u in order:
            z, y, rank = group_peer(u)
            drift_in.append(remote(
                drift.at[h, rank], dstage.at[me * 2 + h], ds_.at[h, u], dr.at[h, u], (z, gx, y)
            ))
        for c in range(3):
            dstage[me * 2 + h, c] = drift[h, me, c]

    for dz in rings:
        arrive(0, dz)
        geometries(0, dz, 0, G)
    pairs(0)
    for dz in rings:
        arrive(1, dz)
        geometries(1, dz, 0, 1)
    pairs(1)

    cross(0, grad, og, esum)
    for h in range(2):
        energy = jnp.sum(esum[0, h], axis=0, keepdims=True) + base[h]
        e0out[h:h + 1, :] = (energy + nuclear[0:1]) * (1.0 / NE)
    e0_in = []
    for u in order:
        z, y, _ = group_peer(u)
        e0_in.append(remote(e0out, e0in.at[me], e0s.at[u], e0r.at[u], (z, gx, y)))
    e0in[me] = e0out[...]

    for dz in rings[:MIDDLE]:
        geometries(1, dz, 1, G)

    for cp in drift_in:
        cp.wait_recv()
    noise_copy.wait()
    for b in range(BLOCKS):
        for c in range(3):
            moved[b, c] = dstage[b, c] + 0.1 * noise_ref[c, :, b * 128:(b + 1) * 128]
    to_smem.wait()

    def pack(q, _):
        for n in range(CAP):
            sendbuf[q * CAP + n] = moved[table[4 + 4 * n + q // 4, lax.rem(q, 4) * 32 + 31]]
        return 0

    lax.fori_loop(0, N_GX, pack, 0)
    blocks_in = []
    for u in range(1, N_GX):
        q = lax.rem(gx + u, N_GX)
        blocks_in.append(remote(
            sendbuf.at[pl.ds(q * CAP, CAP)], recvbuf.at[pl.ds(gx * CAP, CAP)],
            bs.at[u], br.at[u], (gz, q, gy),
        ))
    for n in range(CAP):
        for c in range(3):
            recvbuf[gx * CAP + n, c] = sendbuf[gx * CAP + n, c]

    for cp in e0_in:
        cp.wait_recv()
    for s in range(GROUP):
        for h in range(2):
            kept[2 * s + h, 0:1, :] = e0in[s, h:h + 1, :]
            kept[2 * s + h, 1:2, :] = aw_ref[2 * s + h:2 * s + h + 1, :]

    def packw(q, _):
        for n in range(CAP):
            wout[q, 2 * n:2 * n + 2, :] = kept[table[4 + 4 * n + q // 4, lax.rem(q, 4) * 32 + 31]][0:2]
        return 0

    lax.fori_loop(0, N_GX, packw, 0)
    w_in = []
    for u in range(1, N_GX):
        q = lax.rem(gx + u, N_GX)
        w_in.append(remote(wout.at[q], win.at[gx], ws.at[u], wr.at[u], (gz, q, gy)))
    win[gx] = wout[gx]

    for dz in rings[MIDDLE:]:
        geometries(1, dz, 1, G)
    lax.fori_loop(1, G, lambda g, _: (cross(g, grad, og, esum), 0)[1], 0)

    num = jnp.zeros((G, 128), f32)
    den = jnp.zeros((G, 128), f32)
    for h in range(2):
        for g in range(G):
            erow[h, g:g + 1, :] = jnp.sum(esum[g, h], axis=0, keepdims=True) + base[h]
            lrow[h, g:g + 1, :] = jnp.sum(lsum[g, h], axis=0, keepdims=True)
        le = (erow[h] + nuclear) * (1.0 / NE)
        logs = lrow[h]
        omega = aw_ref[pl.ds(me * 2 + h, 1), :] * jnp.exp(2.0 * (logs - logs[0:1]))
        num = num + omega * le
        den = den + omega
        for z in range(GZ):
            erows[z, h * HIGH:(h + 1) * HIGH, :] = le[z * HIGH:(z + 1) * HIGH]
    lane = lax.broadcasted_iota(i32, (G, 128), 1)
    sub = lax.broadcasted_iota(i32, (G, 128), 0)
    both = jnp.where(lane == sub, jnp.sum(num, axis=1, keepdims=True), 0.0) + jnp.where(
        lane == sub + G, jnp.sum(den, axis=1, keepdims=True), 0.0
    )
    sumrow[...] = jnp.sum(both, axis=0, keepdims=True)
    part_in = []
    rows_in = []
    for u in order:
        z, y, _ = group_peer(u)
        part_in.append(remote(sumrow, sums_in.at[me], ss.at[u], sr.at[u], (z, gx, y)))
    for u in order:
        z, y, _ = group_peer(u)
        rows_in.append(remote(erows.at[z], erows_in.at[me], es.at[u], er.at[u], (z, gx, y)))
    sums_in[me] = sumrow[...]
    erows_in[me] = erows[gz]
    for cp in part_in:
        cp.wait_recv()
    total = sums_in[0]
    for s in range(1, GROUP):
        total = total + sums_in[s]
    allrow[...] = total
    all_parts = []
    for u in range(1, N_GX):
        q = lax.rem(gx + u, N_GX)
        all_parts.append(remote(allrow, all_in.at[gx], gs.at[u], gr.at[u], (gz, q, gy)))
    all_in[gx] = allrow[...]
    for cp in rows_in:
        cp.wait_recv()
    for s in range(GROUP):
        for h in range(2):
            le_ref[:, s * 256 + h * 128:s * 256 + (h + 1) * 128] = erows_in[s, h * HIGH:(h + 1) * HIGH, :]
    for cp in blocks_in:
        cp.wait_recv()
    for d in range(BLOCKS):
        block = recvbuf[table[gx // 4, lax.rem(gx, 4) * 32 + d]]
        for c in range(3):
            np_ref[c, :, d * 128:(d + 1) * 128] = block[c]
    for cp in w_in:
        cp.wait_recv()
    for q in range(N_GX):
        for n in range(CAP):
            kept_in = win[q, 2 * n:2 * n + 2, :]
            arrived[q * CAP + n, 0:2, :] = kept_in
    for cp in all_parts:
        cp.wait_recv()
    whole = all_in[0]
    for q in range(1, N_GX):
        whole = whole + all_in[q]
    estimate = whole / jnp.where(lane_row < G, pltpu.roll(whole, 128 - G, 1), 1.0)
    est_ref[...] = jnp.where(gz == 0, estimate, pltpu.roll(estimate, 128 - HIGH, 1))
    first = estimate[0:1, 0:1]
    for d in range(BLOCKS):
        pair = arrived[table[gx // 4, lax.rem(gx, 4) * 32 + d]]
        nw_ref[d:d + 1, :] = pair[1:2] * jnp.exp(first - pair[0:1])
    for cp in sent:
        cp.wait_send()


def local(
    positions, diffusion_noise, base_nuclei, displacements, charges, orbital_decay,
    coefficients, weights, counts, branch_source,
):
    vmem = pl.BlockSpec(memory_space=pltpu.VMEM)
    smem = pl.BlockSpec(memory_space=pltpu.SMEM)
    hbm = pl.BlockSpec(memory_space=pltpu.HBM)
    dma = pltpu.SemaphoreType.DMA
    v = lambda *shape: pltpu.VMEM(shape, f32)
    le, est, new_pos, new_w = pl.pallas_call(
        step_kernel,
        out_shape=(
            jax.ShapeDtypeStruct((HIGH, GROUP * 256), f32),
            jax.ShapeDtypeStruct((1, 128), f32),
            jax.ShapeDtypeStruct((3, 8, GROUP * 256), f32),
            jax.ShapeDtypeStruct((BLOCKS, BLK), f32),
        ),
        in_specs=[hbm, hbm, smem, smem, smem, smem, smem, vmem, smem, vmem],
        out_specs=(vmem,) * 4,
        scratch_shapes=[
            v(3, 8, GROUP * 256), v(3, 8, GROUP * 256), v(2, 3, 128, 128), v(2, 3, 256, 128),
            v(8, 3, 27 * 8, 128), v(2, 3, 128, 128), v(G, NA, 3, 8, 128), v(NA, 5, 8, 128), v(NA, 3, 8, 128),
            v(G, 2, 3, 128, 128), v(G, 2, 8, 128), v(G, 2, 8, 128), v(2, G, 128), v(2, G, 128),
            v(2, GROUP, 3, 8, 128), v(BLOCKS, 3, 8, 128), v(N_GX * CAP, 3, 8, 128), v(N_GX * CAP, 3, 8, 128),
            v(BLOCKS, 3, 8, 128), v(2, 128), v(GROUP, 2, 128), v(BLOCKS, 8, 128), v(N_GX * CAP, 8, 128),
            v(N_GX, 8, 128), v(N_GX, 8, 128), v(1, 128), v(GROUP, 1, 128), v(GZ, 8, 128), v(GROUP, 8, 128),
            v(1, 128), v(N_GX, 1, 128), v(BLOCKS, BLK),
            pltpu.VMEM((24, 128), i32), pltpu.SMEM((24, 128), i32), dma, dma, dma,
            dma((2, GROUP)), dma((2, GROUP)), dma((2, GROUP)), dma((2, GROUP)), dma((GROUP,)), dma((GROUP,)),
            dma((N_GX,)), dma((N_GX,)), dma((N_GX,)), dma((N_GX,)), dma((GROUP,)), dma((GROUP,)),
            dma((GROUP,)), dma((GROUP,)), dma((N_GX,)), dma((N_GX,)),
        ],
        compiler_params=pltpu.CompilerParams(
            collective_id=0, has_side_effects=True, vmem_limit_bytes=40 * 2**20
        ),
    )(
        positions.transpose(1, 0, 2), diffusion_noise.transpose(1, 0, 2), base_nuclei.T, displacements.transpose(2, 0, 1),
        charges, orbital_decay, coefficients, weights.reshape(BLOCKS, BLK), counts,
        branch_source.reshape(4, 128),
    )
    return le, est[0, :HIGH], new_pos.transpose(1, 0, 2), new_w.reshape(-1)


def solution(mesh):
    placed = (
        P(("gz", "gy"), None, "gx"), P(("gz", "gy"), None, "gx"), P(), P(), P(), P(), P(),
        P("gx"), P("gx"), P(),
    )
    return jax.shard_map(
        local,
        mesh=mesh,
        in_specs=placed,
        out_specs=(P("gz", "gx"), P("gz"), P(("gz", "gy"), None, "gx"), P("gx")),
        check_vma=False,
    )
```

```python
import functools
import math

import jax
import jax.numpy as jnp
from jax import lax
from jax.experimental import pallas as pl
from jax.experimental.pallas import tpu as pltpu
from jax.sharding import PartitionSpec as P

NE = 128
NA = 16
G = 8
BLK = 128
GZ = 2
GY = 8
N_GX = 16
GROUP = GZ * GY
BLOCKS = 2 * GROUP
CAP = 4
f32 = jnp.float32
i32 = jnp.int32
TILES = NE // 8
EARLY = 4
MIDDLE = 8
LOG2E = math.log2(math.e)
HIGH = G // GZ


def rows_at(start):
    return pl.ds(pl.multiple_of(start, 8), 8)


def constants(base_ref, disp_ref, charge_ref, decay_ref, coef_ref, cc, kc):
    def per_atom(a, _):
        for c in range(3):
            for g in range(G):
                cc[g, a, c] = jnp.full((8, 128), (base_ref[c, a] + disp_ref[c, g, a]) * 5.0, f32)
        al = decay_ref[a] * 0.2
        for i, s in enumerate((al * -LOG2E, coef_ref[a], al, al * al, charge_ref[a])):
            kc[a, i] = jnp.full((8, 128), s, f32)
        return 0

    lax.fori_loop(0, NA, per_atom, 0)


def repulsion(cc, kc, nuc):
    sub = lax.broadcasted_iota(jnp.int32, (8, 128), 0)

    def gather(a, _):
        for c in range(3):
            value = cc[0, a, c]
            for g in range(1, G):
                value = jnp.where(sub == g, cc[g, a, c], value)
            nuc[a, c] = value
        return 0

    lax.fori_loop(0, NA, gather, 0)

    def repel(a, total):
        for b in range(1, NA):
            far = b > a
            dx, dy, dz = (nuc[a, c] - nuc[b, c] for c in range(3))
            q = kc[a, 4] * kc[b, 4] * jnp.where(far, f32(1), f32(0))
            d2 = dx * dx + dy * dy + dz * dz + jnp.where(far, f32(0), f32(1))
            total = total + q * lax.rsqrt(d2)
        return total

    return 5.0 * lax.fori_loop(0, NA - 1, repel, jnp.zeros((8, 128), f32))


def take_tile(h, tile, posbuf, pbuf):
    for c in range(3):
        p = posbuf[h, c, rows_at(tile * 8), :] * 5.0
        pbuf[h, c, rows_at(tile * 8), :] = p
        pbuf[h, c, rows_at(tile * 8 + 128), :] = p


def orbital_tiles(at, g, pbuf, cc, kc, og, esum, lsum):
    zero = jnp.zeros((8, 128), f32)
    acc = [[zero] * 6 for _ in at]
    for a in range(NA):
        cx, cy, cz = (cc[g, a, c] for c in range(3))
        na, co, al, a2, ch = (kc[a, i] for i in range(5))
        for i, (h, rank) in enumerate(at):
            ph, gx, gy, gz, la, po = acc[i]
            vx = pbuf[h, 0, rows_at(rank * 8), :] - cx
            vy = pbuf[h, 1, rows_at(rank * 8), :] - cy
            vz = pbuf[h, 2, rows_at(rank * 8), :] - cz
            d2 = (vx * vx + 1.0) + (vy * vy + vz * vz)
            r = lax.rsqrt(d2)
            ex = co * jnp.exp2(na * (d2 * r))
            w = ex * (al * r)
            t2 = r * (r + al) + 2.0
            acc[i] = [ph + ex, gx + w * vx, gy + w * vy, gz + w * vz, la + (a2 * ex - w * t2), po + ch * r]
    for i, (h, rank) in enumerate(at):
        ph, gx, gy, gz, la, po = acc[i]
        inv = 1.0 / ph
        for c, m in enumerate((gx, gy, gz)):
            og[g, h, c, rows_at(rank * 8), :] = m * inv
        esum[g, h] += -12.5 * (la * inv) - 5.0 * po
        lsum[g, h] += jnp.log(ph)


def pair_column(h, t, pbuf, jacc, grad, psum):
    zero = jnp.zeros((8, 128), f32)
    lap, co = psum[h, 0], psum[h, 1]
    back = [[zero] * 3 for _ in range(8)]
    for i in range(8):
        m = 7 - i
        tile = t + 8 + i
        xi, yi, zi = (pbuf[h, c, rows_at(tile * 8), :] for c in range(3))
        gx, gy, gz = zero, zero, zero
        for s in range(1 if m == 0 else 0, 8):
            row = (t - 1) * 8 + s
            dx = xi - pbuf[h, 0, pl.ds(row, 8), :]
            dy = yi - pbuf[h, 1, pl.ds(row, 8), :]
            dz = zi - pbuf[h, 2, pl.ds(row, 8), :]
            r, c, part = pair_terms(dx, dy, dz)
            cx, cy, cz = c * dx, c * dy, c * dz
            back[s] = [back[s][0] + cx, back[s][1] + cy, back[s][2] + cz]
            gx, gy, gz = gx + cx, gy + cy, gz + cz
            lap = lap + part
            co = co + r
        at = rows_at(lax.rem(tile, TILES) * 8)
        grad[h, 0, at, :] += gx
        grad[h, 1, at, :] += gy
        grad[h, 2, at, :] += gz
    for s in range(8):
        for c in range(3):
            jacc[s, c, rows_at(t * 8), :] = back[s][c]
    psum[h, 0] = lap
    psum[h, 1] = co


def pair_terms(dx, dy, dz):
    d2 = (dx * dx + 1.0) + (dy * dy + dz * dz)
    r = lax.rsqrt(d2)
    q = d2 * r + 5.0
    t = lax.rsqrt(q * q)
    c = t * t * r
    return r, c, c * (t * (r + 5.0) + 0.5 * (r * r))


def pair_end(h, pbuf, jacc, grad, psum):
    zero = jnp.zeros((8, 128), f32)

    def opposite(tile, acc):
        lap, co = acc
        near, far = rows_at(tile * 8), rows_at(tile * 8 + 64)
        dx, dy, dz = (pbuf[h, c, near, :] - pbuf[h, c, far, :] for c in range(3))
        r, c, part = pair_terms(dx, dy, dz)
        for k, v in enumerate((dx, dy, dz)):
            grad[h, k, near, :] += c * v
            grad[h, k, far, :] -= c * v
        return lap + part, co + r

    lap, co = lax.fori_loop(0, 8, opposite, (psum[h, 0], psum[h, 1]), unroll=True)
    for s in range(8):
        for c in range(3):
            jacc[s, c, 0:8, :] = jacc[s, c, 128:136, :]

    def fold(tile, jj):
        for c in range(3):
            g = grad[h, c, rows_at(tile * 8), :]
            for s in range(8):
                g = g - jacc[s, c, pl.ds(tile * 8 + (8 - s), 8), :]
            grad[h, c, rows_at(tile * 8), :] = g
            jj = jj + g * g
        return jj

    jj = lax.fori_loop(0, TILES, fold, zero)
    return jnp.sum(5.0 * co - 125.0 * lap - 78.125 * jj, axis=0, keepdims=True)


def cross(g, grad, og, esum):
    for h in range(2):
        acc = jnp.zeros((8, 128), f32)
        for t in range(TILES):
            dot = og[g, h, 0, rows_at(t * 8), :] * grad[h, 0, rows_at(t * 8), :]
            for c in (1, 2):
                dot = dot + og[g, h, c, rows_at(t * 8), :] * grad[h, c, rows_at(t * 8), :]
            acc = acc + dot
        esum[g, h] += 62.5 * acc


def exchange_tables(gx, source_ref, vtable):
    source = source_ref[...]
    device = source // BLOCKS
    lane = lax.broadcasted_iota(i32, (4, 128), 1) % BLOCKS
    rank = jnp.zeros((4, 128), i32)
    for j in range(1, BLOCKS):
        same = (pltpu.roll(device, j, 1) == device) & (lane >= j)
        rank = rank + jnp.where(same, 1, 0)
    vtable[0:4, :] = device * CAP + rank
    for n in range(CAP):
        pick = jnp.where((device == gx) & (rank == n), source % BLOCKS, 0)
        for j in (1, 2, 4, 8, 16):
            pick = pick + pltpu.roll(pick, j, 1)
        vtable[4 + 4 * n:8 + 4 * n, :] = pick


def step_kernel(
    pos_hbm, noise_hbm, base_ref, disp_ref, charge_ref, decay_ref, coef_ref, w_ref, count_ref, source_ref,
    le_ref, est_ref, np_ref, nw_ref,
    pos_ref, noise_ref, posbuf, pbuf, jacc, grad, cc, kc, nuc, og, esum, lsum, erow, lrow, drift, dstage,
    sendbuf, recvbuf, moved, e0out, e0in, kept, arrived, wout, win, sumrow, sums_in, erows, erows_in, allrow, all_in, psum,
    aw_ref, vtable, table, ts, tp, tn,
    ps, pr, ds_, dr, e0s, e0r, bs, br, ws, wr, ss, sr, es, er, gs, gr,
):
    gz = lax.axis_index("gz")
    gx = lax.axis_index("gx")
    gy = lax.axis_index("gy")
    me = gz * GY + gy
    rings = sorted(range(GY), key=lambda u: min(u, GY - u))
    arrival = [0, GY] + [u for dz in rings[1:] for u in (dz, GY + dz)]
    order = arrival[1:]

    def group_peer(u):
        z = lax.rem(gz + u // GY, GZ)
        y = lax.rem(gy + u % GY, GY)
        return z, y, z * GY + y

    def source_rank(u):
        z = lax.rem(gz + GZ - u // GY, GZ)
        return z * GY + lax.rem(gy + GY - u % GY, GY)

    def remote(src, dst, send, recv, peer):
        cp = pltpu.make_async_remote_copy(
            src_ref=src, dst_ref=dst, send_sem=send, recv_sem=recv,
            device_id=peer, device_id_type=pl.DeviceIdType.MESH,
        )
        cp.start()
        sent.append(cp)
        return cp

    sent = []
    pos_copy = pltpu.make_async_copy(pos_hbm, pos_ref, tp)
    pos_copy.start()
    noise_copy = pltpu.make_async_copy(noise_hbm, noise_ref, tn)
    noise_copy.start()
    barrier = pltpu.get_barrier_semaphore()
    for u in order:
        z, y, _ = group_peer(u)
        pl.semaphore_signal(barrier, inc=1, device_id=(z, gx, y), device_id_type=pl.DeviceIdType.MESH)
    for u in range(1, N_GX):
        pl.semaphore_signal(
            barrier, inc=1, device_id=(gz, lax.rem(gx + u, N_GX), gy), device_id_type=pl.DeviceIdType.MESH
        )
    constants(base_ref, disp_ref, charge_ref, decay_ref, coef_ref, cc, kc)
    esum[...] = jnp.zeros_like(esum)
    lsum[...] = jnp.zeros_like(lsum)
    exchange_tables(gx, source_ref, vtable)
    to_smem = pltpu.make_async_copy(vtable, table, ts)
    to_smem.start()
    lane_row = lax.broadcasted_iota(i32, (1, 128), 1)
    for b in range(BLOCKS):
        alive = jnp.where(lane_row < count_ref[b], 1.0, 0.0)
        aw_ref[b:b + 1, :] = w_ref[b:b + 1, :] * alive
    pos_copy.wait()
    for h in range(2):
        posbuf[h, :, 0:8, :] = pos_ref[:, :, pl.ds(pl.multiple_of(me * 256 + h * 128, 128), 128)]
        take_tile(h, 0, posbuf, pbuf)
    grad[...] = jnp.zeros_like(grad)
    psum[...] = jnp.zeros_like(psum)

    def geometries(at, first, last):
        def one(g, _):
            orbital_tiles(at, g, pbuf, cc, kc, og, esum, lsum)
            return 0

        lax.fori_loop(first, last, one, 0)

    geometries([(0, 0), (1, 0)], 0, G)
    nuclear = repulsion(cc, kc, nuc)
    pl.semaphore_wait(barrier, GROUP + N_GX - 2)

    pos_in = {}
    for h in range(2):
        for u in order:
            z, y, rank = group_peer(u)
            pos_in[u, h] = remote(
                pos_ref.at[:, :, pl.ds(pl.multiple_of(rank * 256 + h * 128, 128), 128)],
                posbuf.at[h, :, pl.ds(arrival.index(u) * 8, 8), :],
                ps.at[h, u], pr.at[h, u], (z, gx, y),
            )

    def arrive(h, k):
        pos_in[arrival[k], h].wait_recv()
        take_tile(h, k, posbuf, pbuf)

    def columns(h, first, last):
        def one(t, _):
            pair_column(h, t, pbuf, jacc, grad, psum)
            return 0

        lax.fori_loop(first, last, one, 0)

    base = []
    drift_in = []

    def pairs(h):
        base.append(pair_end(h, pbuf, jacc, grad, psum))
        for k in range(TILES):
            at = slice(k * 8, (k + 1) * 8)
            rank = source_rank(arrival[k])
            for c in range(3):
                drift[h, rank, c] = 0.2 * pbuf[h, c, at, :] + (
                    0.125 * grad[h, c, at, :] - 0.05 * og[0, h, c, at, :]
                )
        for u in order:
            z, y, rank = group_peer(u)
            drift_in.append(remote(
                drift.at[h, rank], dstage.at[me * 2 + h], ds_.at[h, u], dr.at[h, u], (z, gx, y)
            ))
        for c in range(3):
            dstage[me * 2 + h, c] = drift[h, me, c]

    for h in range(2):
        arrive(h, 1)
    geometries([(0, 1), (1, 1)], 0, G)
    for j in range(1, GY):
        arrive(0, 2 * j)
        arrive(0, 2 * j + 1)
        geometries([(0, 2 * j), (0, 2 * j + 1)], 0, G if j <= EARLY else 1)
        if j >= 4:
            columns(0, 2 * j, 2 * j + 2)
    columns(0, 1, 8)
    columns(0, 16, 17)
    pairs(0)
    for j in range(1, GY):
        arrive(1, 2 * j)
        arrive(1, 2 * j + 1)
        geometries([(1, 2 * j), (1, 2 * j + 1)], 0, 1)
    columns(1, 1, 17)
    pairs(1)

    cross(0, grad, og, esum)
    for h in range(2):
        energy = jnp.sum(esum[0, h], axis=0, keepdims=True) + base[h]
        e0out[h:h + 1, :] = (energy + nuclear[0:1]) * (1.0 / NE)
    e0_in = []
    for u in order:
        z, y, _ = group_peer(u)
        e0_in.append(remote(e0out, e0in.at[me], e0s.at[u], e0r.at[u], (z, gx, y)))
    e0in[me] = e0out[...]

    rest = [(0, j) for j in range(EARLY + 1, GY)] + [(1, j) for j in range(1, GY)]
    for h, j in rest[:MIDDLE]:
        geometries([(h, 2 * j), (h, 2 * j + 1)], 1, G)

    for cp in drift_in:
        cp.wait_recv()
    noise_copy.wait()
    for b in range(BLOCKS):
        for c in range(3):
            moved[b, c] = dstage[b, c] + 0.1 * noise_ref[c, :, b * 128:(b + 1) * 128]
    to_smem.wait()

    def pack(q, _):
        for n in range(CAP):
            sendbuf[q * CAP + n] = moved[table[4 + 4 * n + q // 4, lax.rem(q, 4) * 32 + 31]]
        return 0

    lax.fori_loop(0, N_GX, pack, 0)
    blocks_in = []
    for u in range(1, N_GX):
        q = lax.rem(gx + u, N_GX)
        blocks_in.append(remote(
            sendbuf.at[pl.ds(q * CAP, CAP)], recvbuf.at[pl.ds(gx * CAP, CAP)],
            bs.at[u], br.at[u], (gz, q, gy),
        ))
    for n in range(CAP):
        for c in range(3):
            recvbuf[gx * CAP + n, c] = sendbuf[gx * CAP + n, c]

    for cp in e0_in:
        cp.wait_recv()
    for s in range(GROUP):
        for h in range(2):
            kept[2 * s + h, 0:1, :] = e0in[s, h:h + 1, :]
            kept[2 * s + h, 1:2, :] = aw_ref[2 * s + h:2 * s + h + 1, :]

    def packw(q, _):
        for n in range(CAP):
            wout[q, 2 * n:2 * n + 2, :] = kept[table[4 + 4 * n + q // 4, lax.rem(q, 4) * 32 + 31]][0:2]
        return 0

    lax.fori_loop(0, N_GX, packw, 0)
    w_in = []
    for u in range(1, N_GX):
        q = lax.rem(gx + u, N_GX)
        w_in.append(remote(wout.at[q], win.at[gx], ws.at[u], wr.at[u], (gz, q, gy)))
    win[gx] = wout[gx]

    for h, j in rest[MIDDLE:]:
        geometries([(h, 2 * j), (h, 2 * j + 1)], 1, G)
    lax.fori_loop(1, G, lambda g, _: (cross(g, grad, og, esum), 0)[1], 0)

    num = jnp.zeros((G, 128), f32)
    den = jnp.zeros((G, 128), f32)
    for h in range(2):
        for g in range(G):
            erow[h, g:g + 1, :] = jnp.sum(esum[g, h], axis=0, keepdims=True) + base[h]
            lrow[h, g:g + 1, :] = jnp.sum(lsum[g, h], axis=0, keepdims=True)
        le = (erow[h] + nuclear) * (1.0 / NE)
        logs = lrow[h]
        omega = aw_ref[pl.ds(me * 2 + h, 1), :] * jnp.exp(2.0 * (logs - logs[0:1]))
        num = num + omega * le
        den = den + omega
        for z in range(GZ):
            erows[z, h * HIGH:(h + 1) * HIGH, :] = le[z * HIGH:(z + 1) * HIGH]
    lane = lax.broadcasted_iota(i32, (G, 128), 1)
    sub = lax.broadcasted_iota(i32, (G, 128), 0)
    both = jnp.where(lane == sub, jnp.sum(num, axis=1, keepdims=True), 0.0) + jnp.where(
        lane == sub + G, jnp.sum(den, axis=1, keepdims=True), 0.0
    )
    sumrow[...] = jnp.sum(both, axis=0, keepdims=True)
    part_in = []
    rows_in = []
    for u in order:
        z, y, _ = group_peer(u)
        part_in.append(remote(sumrow, sums_in.at[me], ss.at[u], sr.at[u], (z, gx, y)))
    for u in order:
        z, y, _ = group_peer(u)
        rows_in.append(remote(erows.at[z], erows_in.at[me], es.at[u], er.at[u], (z, gx, y)))
    sums_in[me] = sumrow[...]
    erows_in[me] = erows[gz]
    for cp in part_in:
        cp.wait_recv()
    total = sums_in[0]
    for s in range(1, GROUP):
        total = total + sums_in[s]
    allrow[...] = total
    all_parts = []
    for u in range(1, N_GX):
        q = lax.rem(gx + u, N_GX)
        all_parts.append(remote(allrow, all_in.at[gx], gs.at[u], gr.at[u], (gz, q, gy)))
    all_in[gx] = allrow[...]
    for cp in rows_in:
        cp.wait_recv()
    for s in range(GROUP):
        for h in range(2):
            le_ref[:, s * 256 + h * 128:s * 256 + (h + 1) * 128] = erows_in[s, h * HIGH:(h + 1) * HIGH, :]
    for cp in blocks_in:
        cp.wait_recv()
    for d in range(BLOCKS):
        block = recvbuf[table[gx // 4, lax.rem(gx, 4) * 32 + d]]
        for c in range(3):
            np_ref[c, :, d * 128:(d + 1) * 128] = block[c]
    for cp in w_in:
        cp.wait_recv()
    for q in range(N_GX):
        for n in range(CAP):
            kept_in = win[q, 2 * n:2 * n + 2, :]
            arrived[q * CAP + n, 0:2, :] = kept_in
    for cp in all_parts:
        cp.wait_recv()
    whole = all_in[0]
    for q in range(1, N_GX):
        whole = whole + all_in[q]
    estimate = whole / jnp.where(lane_row < G, pltpu.roll(whole, 128 - G, 1), 1.0)
    est_ref[...] = jnp.where(gz == 0, estimate, pltpu.roll(estimate, 128 - HIGH, 1))
    first = estimate[0:1, 0:1]
    for d in range(BLOCKS):
        pair = arrived[table[gx // 4, lax.rem(gx, 4) * 32 + d]]
        nw_ref[d:d + 1, :] = pair[1:2] * jnp.exp(first - pair[0:1])
    for cp in sent:
        cp.wait_send()


def local(
    positions, diffusion_noise, base_nuclei, displacements, charges, orbital_decay,
    coefficients, weights, counts, branch_source,
):
    vmem = pl.BlockSpec(memory_space=pltpu.VMEM)
    smem = pl.BlockSpec(memory_space=pltpu.SMEM)
    hbm = pl.BlockSpec(memory_space=pltpu.HBM)
    dma = pltpu.SemaphoreType.DMA
    v = lambda *shape: pltpu.VMEM(shape, f32)
    le, est, new_pos, new_w = pl.pallas_call(
        step_kernel,
        out_shape=(
            jax.ShapeDtypeStruct((HIGH, GROUP * 256), f32),
            jax.ShapeDtypeStruct((1, 128), f32),
            jax.ShapeDtypeStruct((3, 8, GROUP * 256), f32),
            jax.ShapeDtypeStruct((BLOCKS, BLK), f32),
        ),
        in_specs=[hbm, hbm, smem, smem, smem, smem, smem, vmem, smem, vmem],
        out_specs=(vmem,) * 4,
        scratch_shapes=[
            v(3, 8, GROUP * 256), v(3, 8, GROUP * 256), v(2, 3, 128, 128), v(2, 3, 256, 128),
            v(8, 3, 17 * 8, 128), v(2, 3, 128, 128), v(G, NA, 3, 8, 128), v(NA, 5, 8, 128), v(NA, 3, 8, 128),
            v(G, 2, 3, 128, 128), v(G, 2, 8, 128), v(G, 2, 8, 128), v(2, G, 128), v(2, G, 128),
            v(2, GROUP, 3, 8, 128), v(BLOCKS, 3, 8, 128), v(N_GX * CAP, 3, 8, 128), v(N_GX * CAP, 3, 8, 128),
            v(BLOCKS, 3, 8, 128), v(2, 128), v(GROUP, 2, 128), v(BLOCKS, 8, 128), v(N_GX * CAP, 8, 128),
            v(N_GX, 8, 128), v(N_GX, 8, 128), v(1, 128), v(GROUP, 1, 128), v(GZ, 8, 128), v(GROUP, 8, 128),
            v(1, 128), v(N_GX, 1, 128), v(2, 2, 8, 128), v(BLOCKS, BLK),
            pltpu.VMEM((24, 128), i32), pltpu.SMEM((24, 128), i32), dma, dma, dma,
            dma((2, GROUP)), dma((2, GROUP)), dma((2, GROUP)), dma((2, GROUP)), dma((GROUP,)), dma((GROUP,)),
            dma((N_GX,)), dma((N_GX,)), dma((N_GX,)), dma((N_GX,)), dma((GROUP,)), dma((GROUP,)),
            dma((GROUP,)), dma((GROUP,)), dma((N_GX,)), dma((N_GX,)),
        ],
        compiler_params=pltpu.CompilerParams(
            collective_id=0, has_side_effects=True, vmem_limit_bytes=67043328
        ),
    )(
        positions.transpose(1, 0, 2), diffusion_noise.transpose(1, 0, 2), base_nuclei.T, displacements.transpose(2, 0, 1),
        charges, orbital_decay, coefficients, weights.reshape(BLOCKS, BLK), counts,
        branch_source.reshape(4, 128),
    )
    return le, est[0, :HIGH], new_pos.transpose(1, 0, 2), new_w.reshape(-1)


def solution(mesh):
    placed = (
        P(("gz", "gy"), None, "gx"), P(("gz", "gy"), None, "gx"), P(), P(), P(), P(), P(),
        P("gx"), P("gx"), P(),
    )
    return jax.shard_map(
        local,
        mesh=mesh,
        in_specs=placed,
        out_specs=(P("gz", "gx"), P("gz"), P(("gz", "gy"), None, "gx"), P("gx")),
        check_vma=False,
    )
```

```python
import functools
import math

import jax
import jax.numpy as jnp
from jax import lax
from jax.experimental import pallas as pl
from jax.experimental.pallas import tpu as pltpu
from jax.sharding import PartitionSpec as P

NE = 128
NA = 16
G = 8
BLK = 128
GZ = 2
GY = 8
N_GX = 16
GROUP = GZ * GY
BLOCKS = 2 * GROUP
CAP = 4
f32 = jnp.float32
i32 = jnp.int32
TILES = NE // 8
EARLY = 3
FIRST = 2
SECOND = 5
MIDDLE = 8
LOG2E = math.log2(math.e)
HIGH = G // GZ


def rows_at(start):
    return pl.ds(pl.multiple_of(start, 8), 8)


def constants(base_ref, disp_ref, charge_ref, decay_ref, coef_ref, cc, kc):
    def per_atom(a, _):
        for c in range(3):
            for g in range(G):
                cc[g, a, c] = jnp.full((8, 128), (base_ref[c, a] + disp_ref[c, g, a]) * 5.0, f32)
        for g in range(G):
            x, y, z = (cc[g, a, c] for c in range(3))
            cc[g, a, 3] = x * x + y * y + z * z
        al = decay_ref[a] * 0.2
        for i, s in enumerate((al * -LOG2E, coef_ref[a], al, al * al, charge_ref[a])):
            kc[a, i] = jnp.full((8, 128), s, f32)
        return 0

    lax.fori_loop(0, NA, per_atom, 0)


def repulsion(cc, kc, nuc):
    sub = lax.broadcasted_iota(jnp.int32, (8, 128), 0)

    def gather(a, _):
        for c in range(3):
            value = cc[0, a, c]
            for g in range(1, G):
                value = jnp.where(sub == g, cc[g, a, c], value)
            nuc[a, c] = value
        return 0

    lax.fori_loop(0, NA, gather, 0)

    def repel(a, total):
        for b in range(1, NA):
            far = b > a
            dx, dy, dz = (nuc[a, c] - nuc[b, c] for c in range(3))
            q = kc[a, 4] * kc[b, 4] * jnp.where(far, f32(1), f32(0))
            d2 = dx * dx + dy * dy + dz * dz + jnp.where(far, f32(0), f32(1))
            total = total + q * lax.rsqrt(d2)
        return total

    return 5.0 * lax.fori_loop(0, NA - 1, repel, jnp.zeros((8, 128), f32))


def take_tile(h, tile, posbuf, pbuf):
    for c in range(3):
        p = posbuf[h, c, rows_at(tile * 8), :] * 5.0
        pbuf[h, c, rows_at(tile * 8), :] = p
        pbuf[h, c, rows_at(tile * 8 + 128), :] = p
        pbuf[h, 4 + c, rows_at(tile * 8), :] = -2.0 * p
        square = p * p + (1.0 if c == 0 else square)
    pbuf[h, 3, rows_at(tile * 8), :] = square


def orbital_tiles(at, g, pbuf, cc, kc, og, esum, lsum):
    zero = jnp.zeros((8, 128), f32)
    acc = [[zero] * 7 for _ in at]
    for a in range(NA):
        cx, cy, cz, norm = (cc[g, a, c] for c in range(4))
        na, co, al, a2, ch = (kc[a, i] for i in range(5))
        for i, (h, rank) in enumerate(at):
            ph, w0, mx, my, mz, la, po = acc[i]
            x, y, z = (pbuf[h, 4 + c, rows_at(rank * 8), :] for c in range(3))
            d2 = (pbuf[h, 3, rows_at(rank * 8), :] + norm) + (x * cx + (y * cy + z * cz))
            r = lax.rsqrt(d2)
            ex = co * jnp.exp2(na * (d2 * r))
            s = al * r
            w = ex * s
            acc[i] = [
                ph + ex, w0 + w, mx + w * cx, my + w * cy, mz + w * cz,
                la + (a2 * ex - w * (r * r + s)), po + ch * r,
            ]
    for i, (h, rank) in enumerate(at):
        ph, w0, mx, my, mz, la, po = acc[i]
        inv = 1.0 / ph
        for c, m in enumerate((mx, my, mz)):
            og[g, h, c, rows_at(rank * 8), :] = (pbuf[h, c, rows_at(rank * 8), :] * w0 - m) * inv
        esum[g, h] += -12.5 * ((la - 2.0 * w0) * inv) - 5.0 * po
        lsum[g, h] += jnp.log(ph)


def pair_column(h, t, pbuf, jacc, grad, psum):
    zero = jnp.zeros((8, 128), f32)
    lap, co = psum[h, 0], psum[h, 1]
    back = [[zero] * 3 for _ in range(8)]
    for i in range(8):
        m = 7 - i
        tile = t + 8 + i
        xi, yi, zi = (pbuf[h, c, rows_at(tile * 8), :] for c in range(3))
        gx, gy, gz = zero, zero, zero
        for s in range(1 if m == 0 else 0, 8):
            row = (t - 1) * 8 + s
            dx = xi - pbuf[h, 0, pl.ds(row, 8), :]
            dy = yi - pbuf[h, 1, pl.ds(row, 8), :]
            dz = zi - pbuf[h, 2, pl.ds(row, 8), :]
            r, c, part = pair_terms(dx, dy, dz)
            cx, cy, cz = c * dx, c * dy, c * dz
            back[s] = [back[s][0] + cx, back[s][1] + cy, back[s][2] + cz]
            gx, gy, gz = gx + cx, gy + cy, gz + cz
            lap = lap + part
            co = co + r
        at = rows_at(lax.rem(tile, TILES) * 8)
        grad[h, 0, at, :] += gx
        grad[h, 1, at, :] += gy
        grad[h, 2, at, :] += gz
    for s in range(8):
        for c in range(3):
            jacc[s, c, rows_at(t * 8), :] = back[s][c]
    psum[h, 0] = lap
    psum[h, 1] = co


def pair_terms(dx, dy, dz):
    d2 = (dx * dx + 1.0) + (dy * dy + dz * dz)
    r = lax.rsqrt(d2)
    q = d2 * r + 5.0
    t = lax.rsqrt(q * q)
    c = t * t * r
    return r, c, c * (t * (r + 5.0) + 0.5 * (r * r))


def pair_end(h, pbuf, jacc, grad, psum):
    zero = jnp.zeros((8, 128), f32)

    def opposite(tile, acc):
        lap, co = acc
        near, far = rows_at(tile * 8), rows_at(tile * 8 + 64)
        dx, dy, dz = (pbuf[h, c, near, :] - pbuf[h, c, far, :] for c in range(3))
        r, c, part = pair_terms(dx, dy, dz)
        for k, v in enumerate((dx, dy, dz)):
            grad[h, k, near, :] += c * v
            grad[h, k, far, :] -= c * v
        return lap + part, co + r

    lap, co = lax.fori_loop(0, 8, opposite, (psum[h, 0], psum[h, 1]), unroll=True)
    for s in range(8):
        for c in range(3):
            jacc[s, c, 0:8, :] = jacc[s, c, 128:136, :]

    def fold(tile, jj):
        for c in range(3):
            g = grad[h, c, rows_at(tile * 8), :]
            for s in range(8):
                g = g - jacc[s, c, pl.ds(tile * 8 + (8 - s), 8), :]
            grad[h, c, rows_at(tile * 8), :] = g
            jj = jj + g * g
        return jj

    jj = lax.fori_loop(0, TILES, fold, zero)
    return jnp.sum(5.0 * co - 125.0 * lap - 78.125 * jj, axis=0, keepdims=True)


def cross(g, grad, og, esum):
    for h in range(2):
        acc = jnp.zeros((8, 128), f32)
        for t in range(TILES):
            dot = og[g, h, 0, rows_at(t * 8), :] * grad[h, 0, rows_at(t * 8), :]
            for c in (1, 2):
                dot = dot + og[g, h, c, rows_at(t * 8), :] * grad[h, c, rows_at(t * 8), :]
            acc = acc + dot
        esum[g, h] += 62.5 * acc


def finish_kernel(le_ref, est_ref, np_ref, nw_ref, le_out, est_out, np_out, nw_out):
    le_out[...] = le_ref[...]
    np_out[...] = np_ref[...]
    nw_out[...] = nw_ref[...]
    for g in range(HIGH):
        est_out[g] = est_ref[0, g]


def exchange_tables(gx, source_ref, vtable):
    source = source_ref[...]
    device = source // BLOCKS
    block = source % BLOCKS
    lane = lax.broadcasted_iota(i32, (4, 128), 1)
    sub = lax.broadcasted_iota(i32, (4, 128), 0)
    index = sub * 128 + lane
    rank = jnp.zeros((4, 128), i32)
    for j in range(1, BLOCKS):
        same = (pltpu.roll(device, j, 1) == device) & (lane % BLOCKS >= j)
        rank = rank + jnp.where(same, 1, 0)
    hit = device == gx
    ones = jnp.where(hit, 1, 0)
    before = ones
    for j in (1, 2, 4, 8, 16, 32, 64):
        before = before + jnp.where(lane >= j, pltpu.roll(before, j, 1), 0)
    position = before - ones
    for i in range(3):
        position = position + jnp.where(sub > i, before[i:i + 1, 127:128], 0)

    def over_lanes(rows, pick):
        which = lax.broadcasted_iota(i32, (rows, 128), 0)
        total = pick(0, which)
        for i in range(1, 4):
            total = total + pick(i, which)
        for j in (1, 2, 4, 8, 16, 32, 64):
            total = total + pltpu.roll(total, j, 1)
        return total

    own_position = jnp.where(hit, position, -1)
    own_block = jnp.where(hit, block, -1)
    last = BLOCKS - 1
    vtable[8:40, :] = jnp.minimum(last, over_lanes(
        BLOCKS, lambda i, w: jnp.where(own_position[i:i + 1] == w, block[i:i + 1], 0)
    ))
    vtable[40:72, :] = jnp.minimum(last, over_lanes(
        BLOCKS, lambda i, w: jnp.where(own_block[i:i + 1] == w, position[i:i + 1], 0)
    ))
    vtable[72:88, :] = over_lanes(
        N_GX, lambda i, w: jnp.where(index[i:i + 1] < w * BLOCKS, ones[i:i + 1], 0)
    )
    earlier = over_lanes(
        N_GX, lambda i, w: jnp.where((device[i:i + 1] == w) & (index[i:i + 1] < gx * BLOCKS), 1, 0)
    )
    first = jnp.zeros((4, 128), i32)
    for p in range(N_GX):
        first = first + jnp.where(device == p, earlier[p:p + 1], 0)
    vtable[0:4, :] = ((first + rank) % 2) * BLOCKS + device * 2 + jnp.minimum(rank // 2, 1)


def step_kernel(
    pos_hbm, noise_hbm, base_ref, disp_ref, charge_ref, decay_ref, coef_ref, w_ref, count_ref, source_ref,
    le_ref, est_ref, np_ref, nw_ref,
    pos_ref, noise_ref, posbuf, pbuf, jacc, grad, cc, kc, nuc, og, esum, lsum, erow, lrow, drift, dstage,
    sendbuf, recvbuf, moved, e0out, e0in, kept, arrived, wout, win, sumrow, sums_in, erows, erows_in, allrow, all_in, psum,
    aw_ref, awblock, blocks, possort, vtable, table, ts, tp, tn,
    ps, pr, ds_, dr, e0s, e0r, bs, br, ws, wr, ss, sr, es, er, gs, gr,
):
    gz = lax.axis_index("gz")
    gx = lax.axis_index("gx")
    gy = lax.axis_index("gy")
    me = gz * GY + gy
    rings = sorted(range(GY), key=lambda u: min(u, GY - u))
    arrival = [0, GY] + [u for dz in rings[1:] for u in (dz, GY + dz)]
    order = arrival[1:]

    def group_peer(u):
        z = lax.rem(gz + u // GY, GZ)
        y = lax.rem(gy + u % GY, GY)
        return z, y, z * GY + y

    def source_rank(u):
        z = lax.rem(gz + GZ - u // GY, GZ)
        return z * GY + lax.rem(gy + GY - u % GY, GY)

    def remote(src, dst, send, recv, peer):
        cp = pltpu.make_async_remote_copy(
            src_ref=src, dst_ref=dst, send_sem=send, recv_sem=recv,
            device_id=peer, device_id_type=pl.DeviceIdType.MESH,
        )
        cp.start()
        sent.append(cp)
        return cp

    sent = []
    pos_copy = pltpu.make_async_copy(pos_hbm, pos_ref, tp)
    pos_copy.start()
    noise_copy = pltpu.make_async_copy(noise_hbm, noise_ref, tn)
    noise_copy.start()
    barrier = pltpu.get_barrier_semaphore()
    for u in order:
        z, y, _ = group_peer(u)
        pl.semaphore_signal(barrier, inc=1, device_id=(z, gx, y), device_id_type=pl.DeviceIdType.MESH)
    for u in range(1, N_GX):
        pl.semaphore_signal(
            barrier, inc=1, device_id=(gz, lax.rem(gx + u, N_GX), gy), device_id_type=pl.DeviceIdType.MESH
        )
    exchange_tables(gx, source_ref, vtable)
    to_smem = pltpu.make_async_copy(vtable, table, ts)
    to_smem.start()
    esum[...] = jnp.zeros_like(esum)
    lsum[...] = jnp.zeros_like(lsum)
    lane_row = lax.broadcasted_iota(i32, (1, 128), 1)
    for b in range(BLOCKS):
        alive = jnp.where(lane_row < count_ref[b], 1.0, 0.0)
        awblock[b] = w_ref[b:b + 1, :] * alive
    pos_copy.wait()
    for b in range(BLOCKS):
        for c in range(3):
            blocks[b, c] = pos_ref[c, :, b * 128:(b + 1) * 128]
    to_smem.wait()

    def sort(j, _):
        possort[j] = blocks[table[8 + j, 0]]
        aw_ref[j] = awblock[table[8 + j, 0]]
        return 0

    lax.fori_loop(0, BLOCKS, sort, 0)
    for h in range(2):
        posbuf[h, :, 0:8, :] = possort[me * 2 + h]
        take_tile(h, 0, posbuf, pbuf)
    grad[...] = jnp.zeros_like(grad)
    psum[...] = jnp.zeros_like(psum)

    def geometries(at, first, last):
        def one(g, _):
            orbital_tiles(at, g, pbuf, cc, kc, og, esum, lsum)
            return 0

        lax.fori_loop(first, last, one, 0)

    pl.semaphore_wait(barrier, GROUP + N_GX - 2)

    pos_in = {}
    for h in range(2):
        for u in order:
            z, y, rank = group_peer(u)
            pos_in[u, h] = remote(
                possort.at[rank * 2 + h],
                posbuf.at[h, :, pl.ds(arrival.index(u) * 8, 8), :],
                ps.at[h, u], pr.at[h, u], (z, gx, y),
            )

    constants(base_ref, disp_ref, charge_ref, decay_ref, coef_ref, cc, kc)
    nuclear = repulsion(cc, kc, nuc)

    def arrive(h, k):
        pos_in[arrival[k], h].wait_recv()
        take_tile(h, k, posbuf, pbuf)

    def columns(h, first, last):
        def one(t, _):
            pair_column(h, t, pbuf, jacc, grad, psum)
            return 0

        lax.fori_loop(first, last, one, 0)

    base = []
    drift_in = [[], []]

    e0_in = []

    def early_energies():
        cross(0, grad, og, esum)
        for h in range(2):
            energy = jnp.sum(esum[0, h], axis=0, keepdims=True) + base[h]
            e0out[h:h + 1, :] = (energy + nuclear[0:1]) * (1.0 / NE)
        for u in order:
            z, y, _ = group_peer(u)
            e0_in.append(remote(e0out, e0in.at[me], e0s.at[u], e0r.at[u], (z, gx, y)))
        e0in[me] = e0out[...]

    def pairs(h):
        base.append(pair_end(h, pbuf, jacc, grad, psum))
        if h == 1:
            early_energies()
        for k in range(TILES):
            at = slice(k * 8, (k + 1) * 8)
            rank = source_rank(arrival[k])
            for c in range(3):
                drift[h, rank, c] = 0.2 * pbuf[h, c, at, :] + (
                    0.125 * grad[h, c, at, :] - 0.05 * og[0, h, c, at, :]
                )
        for u in order:
            z, y, rank = group_peer(u)
            drift_in[h].append(remote(
                drift.at[h, rank], dstage.at[me * 2 + h], ds_.at[h, u], dr.at[h, u], (z, gx, y)
            ))
        for c in range(3):
            dstage[me * 2 + h, c] = drift[h, me, c]

    geometries([(0, 0), (1, 0)], 0, G)
    for h in range(2):
        arrive(h, 1)
    geometries([(0, 1), (1, 1)], 0, G)
    for j in range(1, GY):
        arrive(0, 2 * j)
        arrive(0, 2 * j + 1)
        geometries([(0, 2 * j), (0, 2 * j + 1)], 0, G if j <= EARLY else 1)
        if j >= 4:
            columns(0, 2 * j, 2 * j + 2)
    columns(0, 1, 8)
    columns(0, 16, 17)
    pairs(0)
    for j in range(1, GY):
        arrive(1, 2 * j)
        arrive(1, 2 * j + 1)
        geometries([(1, 2 * j), (1, 2 * j + 1)], 0, 1)
    columns(1, 1, 17)
    pairs(1)

    rest = [(0, j) for j in range(EARLY + 1, GY)] + [(1, j) for j in range(1, GY)]
    blocks_in = []

    def pick(q, h, n):
        start = table[72 + q, 0]
        return jnp.minimum(start + lax.rem(start + h, 2) + 2 * n, BLOCKS - 1)

    def exchange_half(h):
        for cp in drift_in[h]:
            cp.wait_recv()

        def move(s, _):
            moved[s * 2 + h] = dstage[s * 2 + h] + 0.1 * blocks[table[8 + s * 2 + h, 0]]
            return 0

        lax.fori_loop(0, GROUP, move, 0)

        def pack(q, _):
            for n in range(2):
                sendbuf[h * BLOCKS + q * 2 + n] = moved[pick(q, h, n)]
            return 0

        lax.fori_loop(0, N_GX, pack, 0)
        for u in range(1, N_GX):
            q = lax.rem(gx + u, N_GX)
            blocks_in.append(remote(
                sendbuf.at[pl.ds(h * BLOCKS + q * 2, 2)], recvbuf.at[pl.ds(h * BLOCKS + gx * 2, 2)],
                bs.at[h, u], br.at[h, u], (gz, q, gy),
            ))
        for n in range(2):
            recvbuf[h * BLOCKS + gx * 2 + n] = sendbuf[h * BLOCKS + gx * 2 + n]

    for h, j in rest[:FIRST]:
        geometries([(h, 2 * j), (h, 2 * j + 1)], 1, G)
    noise_copy.wait()
    for b in range(BLOCKS):
        for c in range(3):
            blocks[b, c] = noise_ref[c, :, b * 128:(b + 1) * 128]
    exchange_half(0)
    for h, j in rest[FIRST:SECOND]:
        geometries([(h, 2 * j), (h, 2 * j + 1)], 1, G)
    for cp in e0_in:
        cp.wait_recv()
    for s in range(GROUP):
        for h in range(2):
            kept[2 * s + h, 0:1, :] = e0in[s, h:h + 1, :]
            kept[2 * s + h, 1:2, :] = aw_ref[2 * s + h]

    def packw(q, _):
        for h in range(2):
            for n in range(2):
                i = 2 * h + n
                wout[q, 2 * i:2 * i + 2, :] = kept[pick(q, h, n)][0:2]
        return 0

    lax.fori_loop(0, N_GX, packw, 0)
    w_in = []
    for u in range(1, N_GX):
        q = lax.rem(gx + u, N_GX)
        w_in.append(remote(wout.at[q], win.at[gx], ws.at[u], wr.at[u], (gz, q, gy)))
    win[gx] = wout[gx]
    for h, j in rest[SECOND:MIDDLE]:
        geometries([(h, 2 * j), (h, 2 * j + 1)], 1, G)
    exchange_half(1)

    for h, j in rest[MIDDLE:]:
        geometries([(h, 2 * j), (h, 2 * j + 1)], 1, G)
    lax.fori_loop(1, G, lambda g, _: (cross(g, grad, og, esum), 0)[1], 0)

    num = jnp.zeros((G, 128), f32)
    den = jnp.zeros((G, 128), f32)
    for h in range(2):
        for g in range(G):
            erow[h, g:g + 1, :] = jnp.sum(esum[g, h], axis=0, keepdims=True) + base[h]
            lrow[h, g:g + 1, :] = jnp.sum(lsum[g, h], axis=0, keepdims=True)
        le = (erow[h] + nuclear) * (1.0 / NE)
        logs = lrow[h]
        omega = aw_ref[me * 2 + h] * jnp.exp(2.0 * (logs - logs[0:1]))
        num = num + omega * le
        den = den + omega
        for z in range(GZ):
            erows[z, h] = le[z * HIGH:(z + 1) * HIGH]
    lane = lax.broadcasted_iota(i32, (G, 128), 1)
    sub = lax.broadcasted_iota(i32, (G, 128), 0)
    both = jnp.where(lane == sub, jnp.sum(num, axis=1, keepdims=True), 0.0) + jnp.where(
        lane == sub + G, jnp.sum(den, axis=1, keepdims=True), 0.0
    )
    sumrow[...] = jnp.sum(both, axis=0, keepdims=True)
    part_in = []
    rows_in = []
    for u in order:
        z, y, _ = group_peer(u)
        part_in.append(remote(sumrow, sums_in.at[me], ss.at[u], sr.at[u], (z, gx, y)))
    for u in order:
        z, y, _ = group_peer(u)
        rows_in.append(remote(erows.at[z], erows_in.at[pl.ds(me * 2, 2)], es.at[u], er.at[u], (z, gx, y)))
    sums_in[me] = sumrow[...]
    erows_in[pl.ds(me * 2, 2)] = erows[gz]
    for cp in part_in:
        cp.wait_recv()
    total = sums_in[0]
    for s in range(1, GROUP):
        total = total + sums_in[s]
    allrow[...] = total
    all_parts = []
    for u in range(1, N_GX):
        q = lax.rem(gx + u, N_GX)
        all_parts.append(remote(allrow, all_in.at[gx], gs.at[u], gr.at[u], (gz, q, gy)))
    all_in[gx] = allrow[...]
    for cp in rows_in:
        cp.wait_recv()
    for b in range(BLOCKS):
        le_ref[:, b * 128:(b + 1) * 128] = erows_in[table[40 + b, 0]]
    for cp in blocks_in:
        cp.wait_recv()
    for d in range(BLOCKS):
        block = recvbuf[table[gx // 4, lax.rem(gx, 4) * 32 + d]]
        for c in range(3):
            np_ref[c, :, d * 128:(d + 1) * 128] = block[c]
    for cp in w_in:
        cp.wait_recv()
    for q in range(N_GX):
        for h in range(2):
            for n in range(2):
                i = 2 * h + n
                arrived[h * BLOCKS + q * 2 + n, 0:2, :] = win[q, 2 * i:2 * i + 2, :]
    for cp in all_parts:
        cp.wait_recv()
    whole = all_in[0]
    for q in range(1, N_GX):
        whole = whole + all_in[q]
    estimate = whole / jnp.where(lane_row < G, pltpu.roll(whole, 128 - G, 1), 1.0)
    est_ref[...] = jnp.where(gz == 0, estimate, pltpu.roll(estimate, 128 - HIGH, 1))
    first = estimate[0:1, 0:1]
    for d in range(BLOCKS):
        pair = arrived[table[gx // 4, lax.rem(gx, 4) * 32 + d]]
        nw_ref[d:d + 1, :] = pair[1:2] * jnp.exp(first - pair[0:1])
    for cp in sent:
        cp.wait_send()


def local(
    positions, diffusion_noise, base_nuclei, displacements, charges, orbital_decay,
    coefficients, weights, counts, branch_source,
):
    vmem = pl.BlockSpec(memory_space=pltpu.VMEM)
    smem = pl.BlockSpec(memory_space=pltpu.SMEM)
    hbm = pl.BlockSpec(memory_space=pltpu.HBM)
    dma = pltpu.SemaphoreType.DMA
    v = lambda *shape: pltpu.VMEM(shape, f32)
    le, est, new_pos, new_w = pl.pallas_call(
        step_kernel,
        out_shape=(
            jax.ShapeDtypeStruct((HIGH, GROUP * 256), f32),
            jax.ShapeDtypeStruct((1, 128), f32),
            jax.ShapeDtypeStruct((3, 8, GROUP * 256), f32),
            jax.ShapeDtypeStruct((BLOCKS, BLK), f32),
        ),
        in_specs=[hbm, hbm, smem, smem, smem, smem, smem, vmem, smem, vmem],
        out_specs=(vmem,) * 4,
        scratch_shapes=[
            v(3, 8, GROUP * 256), v(3, 8, GROUP * 256), v(2, 3, 128, 128), v(2, 7, 256, 128),
            v(8, 3, 17 * 8, 128), v(2, 3, 128, 128), v(G, NA, 4, 8, 128), v(NA, 5, 8, 128), v(NA, 3, 8, 128),
            v(G, 2, 3, 128, 128), v(G, 2, 8, 128), v(G, 2, 8, 128), v(2, G, 128), v(2, G, 128),
            v(2, GROUP, 3, 8, 128), v(BLOCKS, 3, 8, 128), v(N_GX * CAP, 3, 8, 128), v(N_GX * CAP, 3, 8, 128),
            v(BLOCKS, 3, 8, 128), v(2, 128), v(GROUP, 2, 128), v(BLOCKS, 8, 128), v(N_GX * CAP, 8, 128),
            v(N_GX, 8, 128), v(N_GX, 8, 128), v(1, 128), v(GROUP, 1, 128), v(GZ, 2, HIGH, 128), v(BLOCKS, HIGH, 128),
            v(1, 128), v(N_GX, 1, 128), v(2, 2, 8, 128),
            v(BLOCKS, 1, BLK), v(BLOCKS, 1, BLK), v(BLOCKS, 3, 8, 128), v(BLOCKS, 3, 8, 128),
            pltpu.VMEM((88, 128), i32), pltpu.SMEM((88, 128), i32), dma, dma, dma,
            dma((2, GROUP)), dma((2, GROUP)), dma((2, GROUP)), dma((2, GROUP)), dma((GROUP,)), dma((GROUP,)),
            dma((2, N_GX)), dma((2, N_GX)), dma((N_GX,)), dma((N_GX,)), dma((GROUP,)), dma((GROUP,)),
            dma((GROUP,)), dma((GROUP,)), dma((N_GX,)), dma((N_GX,)),
        ],
        compiler_params=pltpu.CompilerParams(
            collective_id=0, has_side_effects=True, vmem_limit_bytes=67043328
        ),
    )(
        positions.transpose(1, 0, 2), diffusion_noise.transpose(1, 0, 2), base_nuclei.T, displacements.transpose(2, 0, 1),
        charges, orbital_decay, coefficients, weights.reshape(BLOCKS, BLK), counts,
        branch_source.reshape(4, 128),
    )
    le, est, new_pos, new_w = pl.pallas_call(
        finish_kernel,
        out_shape=(
            jax.ShapeDtypeStruct(le.shape, f32), jax.ShapeDtypeStruct((HIGH,), f32),
            jax.ShapeDtypeStruct(new_pos.shape, f32), jax.ShapeDtypeStruct(new_w.shape, f32),
        ),
        in_specs=[vmem, smem, vmem, vmem],
        out_specs=(vmem, smem, vmem, vmem),
    )(le, est, new_pos, new_w)
    return le, est, new_pos.transpose(1, 0, 2), new_w.reshape(-1)


def solution(mesh):
    placed = (
        P(("gz", "gy"), None, "gx"), P(("gz", "gy"), None, "gx"), P(), P(), P(), P(), P(),
        P("gx"), P("gx"), P(),
    )
    return jax.shard_map(
        local,
        mesh=mesh,
        in_specs=placed,
        out_specs=(P("gz", "gx"), P("gz"), P(("gz", "gy"), None, "gx"), P("gx")),
        check_vma=False,
    )
```

```python
import functools
import math

import jax
import jax.numpy as jnp
from jax import lax
from jax.experimental import pallas as pl
from jax.experimental.pallas import tpu as pltpu
from jax.sharding import PartitionSpec as P

NE = 128
NA = 16
G = 8
BLK = 128
GZ = 2
GY = 8
N_GX = 16
GROUP = GZ * GY
BLOCKS = 2 * GROUP
CAP = 4
f32 = jnp.float32
i32 = jnp.int32
TILES = NE // 8
EARLY = 3
FIRST = 2
SECOND = 5
MIDDLE = 8
LOG2E = math.log2(math.e)
HIGH = G // GZ


def rows_at(start):
    return pl.ds(pl.multiple_of(start, 8), 8)


def constants(base_ref, disp_ref, charge_ref, decay_ref, coef_ref, cc, kc):
    def per_atom(a, _):
        for c in range(3):
            for g in range(G):
                cc[g, a, c] = jnp.full((8, 128), (base_ref[c, a] + disp_ref[c, g, a]) * 5.0, f32)
        for g in range(G):
            x, y, z = (cc[g, a, c] for c in range(3))
            cc[g, a, 3] = x * x + y * y + z * z
        al = decay_ref[a] * 0.2
        for i, s in enumerate((al * -LOG2E, coef_ref[a], al, al * al, charge_ref[a])):
            kc[a, i] = jnp.full((8, 128), s, f32)
        return 0

    lax.fori_loop(0, NA, per_atom, 0)


def repulsion(cc, kc, nuc):
    sub = lax.broadcasted_iota(jnp.int32, (8, 128), 0)

    def gather(a, _):
        for c in range(3):
            value = cc[0, a, c]
            for g in range(1, G):
                value = jnp.where(sub == g, cc[g, a, c], value)
            nuc[a, c] = value
        return 0

    lax.fori_loop(0, NA, gather, 0)

    def repel(a, total):
        for b in range(1, NA):
            far = b > a
            dx, dy, dz = (nuc[a, c] - nuc[b, c] for c in range(3))
            q = kc[a, 4] * kc[b, 4] * jnp.where(far, f32(1), f32(0))
            d2 = dx * dx + dy * dy + dz * dz + jnp.where(far, f32(0), f32(1))
            total = total + q * lax.rsqrt(d2)
        return total

    return 5.0 * lax.fori_loop(0, NA - 1, repel, jnp.zeros((8, 128), f32))


def take_tile(h, tile, posbuf, pbuf):
    for c in range(3):
        p = posbuf[h, c, rows_at(tile * 8), :] * 5.0
        pbuf[h, c, rows_at(tile * 8), :] = p
        pbuf[h, c, rows_at(tile * 8 + 128), :] = p
        pbuf[h, 4 + c, rows_at(tile * 8), :] = -2.0 * p
        square = p * p + (1.0 if c == 0 else square)
    pbuf[h, 3, rows_at(tile * 8), :] = square


def orbital_tiles(at, g, pbuf, cc, kc, og, esum, lsum):
    zero = jnp.zeros((8, 128), f32)
    acc = [[zero] * 7 for _ in at]
    for a in range(NA):
        cx, cy, cz, norm = (cc[g, a, c] for c in range(4))
        na, co, al, a2, ch = (kc[a, i] for i in range(5))
        for i, (h, rank) in enumerate(at):
            ph, w0, mx, my, mz, la, po = acc[i]
            x, y, z = (pbuf[h, 4 + c, rows_at(rank * 8), :] for c in range(3))
            d2 = (pbuf[h, 3, rows_at(rank * 8), :] + norm) + (x * cx + (y * cy + z * cz))
            r = lax.rsqrt(d2)
            ex = co * jnp.exp2(na * (d2 * r))
            s = al * r
            w = ex * s
            acc[i] = [
                ph + ex, w0 + w, mx + w * cx, my + w * cy, mz + w * cz,
                la + (a2 * ex - w * (r * r + s)), po + ch * r,
            ]
    for i, (h, rank) in enumerate(at):
        ph, w0, mx, my, mz, la, po = acc[i]
        inv = 1.0 / ph
        for c, m in enumerate((mx, my, mz)):
            og[g, h, c, rows_at(rank * 8), :] = (pbuf[h, c, rows_at(rank * 8), :] * w0 - m) * inv
        esum[g, h] += -12.5 * ((la - 2.0 * w0) * inv) - 5.0 * po
        lsum[g, h] += jnp.log(ph)


def pair_column(h, t, pbuf, jacc, grad, psum):
    zero = jnp.zeros((8, 128), f32)
    lap, co = psum[h, 0], psum[h, 1]
    back = [[zero] * 3 for _ in range(8)]
    for i in range(8):
        m = 7 - i
        tile = t + 8 + i
        xi, yi, zi = (pbuf[h, c, rows_at(tile * 8), :] for c in range(3))
        gx, gy, gz = zero, zero, zero
        for s in range(1 if m == 0 else 0, 8):
            row = (t - 1) * 8 + s
            dx = xi - pbuf[h, 0, pl.ds(row, 8), :]
            dy = yi - pbuf[h, 1, pl.ds(row, 8), :]
            dz = zi - pbuf[h, 2, pl.ds(row, 8), :]
            r, c, part = pair_terms(dx, dy, dz)
            cx, cy, cz = c * dx, c * dy, c * dz
            back[s] = [back[s][0] + cx, back[s][1] + cy, back[s][2] + cz]
            gx, gy, gz = gx + cx, gy + cy, gz + cz
            lap = lap + part
            co = co + r
        at = rows_at(lax.rem(tile, TILES) * 8)
        grad[h, 0, at, :] += gx
        grad[h, 1, at, :] += gy
        grad[h, 2, at, :] += gz
    for s in range(8):
        for c in range(3):
            jacc[s, c, rows_at(t * 8), :] = back[s][c]
    psum[h, 0] = lap
    psum[h, 1] = co


def pair_terms(dx, dy, dz):
    d2 = (dx * dx + 1.0) + (dy * dy + dz * dz)
    r = lax.rsqrt(d2)
    q = d2 * r + 5.0
    t = lax.rsqrt(q * q)
    c = t * t * r
    return r, c, c * (t * (r + 5.0) + 0.5 * (r * r))


def pair_end(h, pbuf, jacc, grad, psum):
    zero = jnp.zeros((8, 128), f32)

    def opposite(tile, acc):
        lap, co = acc
        near, far = rows_at(tile * 8), rows_at(tile * 8 + 64)
        dx, dy, dz = (pbuf[h, c, near, :] - pbuf[h, c, far, :] for c in range(3))
        r, c, part = pair_terms(dx, dy, dz)
        for k, v in enumerate((dx, dy, dz)):
            grad[h, k, near, :] += c * v
            grad[h, k, far, :] -= c * v
        return lap + part, co + r

    lap, co = lax.fori_loop(0, 8, opposite, (psum[h, 0], psum[h, 1]), unroll=True)
    for s in range(8):
        for c in range(3):
            jacc[s, c, 0:8, :] = jacc[s, c, 128:136, :]

    def fold(tile, jj):
        for c in range(3):
            g = grad[h, c, rows_at(tile * 8), :]
            for s in range(8):
                g = g - jacc[s, c, pl.ds(tile * 8 + (8 - s), 8), :]
            grad[h, c, rows_at(tile * 8), :] = g
            jj = jj + g * g
        return jj

    jj = lax.fori_loop(0, TILES, fold, zero)
    return jnp.sum(5.0 * co - 125.0 * lap - 78.125 * jj, axis=0, keepdims=True)


def cross(g, grad, og, esum):
    for h in range(2):
        acc = jnp.zeros((8, 128), f32)
        for t in range(TILES):
            dot = og[g, h, 0, rows_at(t * 8), :] * grad[h, 0, rows_at(t * 8), :]
            for c in (1, 2):
                dot = dot + og[g, h, c, rows_at(t * 8), :] * grad[h, c, rows_at(t * 8), :]
            acc = acc + dot
        esum[g, h] += 62.5 * acc


def finish_kernel(le_ref, est_ref, np_ref, nw_ref, le_out, est_out, np_out, nw_out):
    le_out[...] = le_ref[...]
    np_out[...] = np_ref[...]
    nw_out[...] = nw_ref[...]
    for g in range(HIGH):
        est_out[g] = est_ref[0, g]


def exchange_tables(gx, source_ref, vtable):
    source = source_ref[...]
    device = source // BLOCKS
    block = source % BLOCKS
    lane = lax.broadcasted_iota(i32, (4, 128), 1)
    sub = lax.broadcasted_iota(i32, (4, 128), 0)
    index = sub * 128 + lane
    rank = jnp.zeros((4, 128), i32)
    for j in range(1, BLOCKS):
        same = (pltpu.roll(device, j, 1) == device) & (lane % BLOCKS >= j)
        rank = rank + jnp.where(same, 1, 0)
    hit = device == gx
    ones = jnp.where(hit, 1, 0)
    before = ones
    for j in (1, 2, 4, 8, 16, 32, 64):
        before = before + jnp.where(lane >= j, pltpu.roll(before, j, 1), 0)
    position = before - ones
    for i in range(3):
        position = position + jnp.where(sub > i, before[i:i + 1, 127:128], 0)

    def over_lanes(rows, pick):
        which = lax.broadcasted_iota(i32, (rows, 128), 0)
        total = pick(0, which)
        for i in range(1, 4):
            total = total + pick(i, which)
        for j in (1, 2, 4, 8, 16, 32, 64):
            total = total + pltpu.roll(total, j, 1)
        return total

    own_position = jnp.where(hit, position, -1)
    own_block = jnp.where(hit, block, -1)
    last = BLOCKS - 1
    vtable[8:40, :] = jnp.minimum(last, over_lanes(
        BLOCKS, lambda i, w: jnp.where(own_position[i:i + 1] == w, block[i:i + 1], 0)
    ))
    vtable[40:72, :] = jnp.minimum(last, over_lanes(
        BLOCKS, lambda i, w: jnp.where(own_block[i:i + 1] == w, position[i:i + 1], 0)
    ))
    vtable[72:88, :] = over_lanes(
        N_GX, lambda i, w: jnp.where(index[i:i + 1] < w * BLOCKS, ones[i:i + 1], 0)
    )
    earlier = over_lanes(
        N_GX, lambda i, w: jnp.where((device[i:i + 1] == w) & (index[i:i + 1] < gx * BLOCKS), 1, 0)
    )
    first = jnp.zeros((4, 128), i32)
    for p in range(N_GX):
        first = first + jnp.where(device == p, earlier[p:p + 1], 0)
    vtable[0:4, :] = ((first + rank) % 2) * BLOCKS + device * 2 + jnp.minimum(rank // 2, 1)


def step_kernel(
    pos_hbm, noise_hbm, base_ref, disp_ref, charge_ref, decay_ref, coef_ref, w_ref, count_ref, source_ref,
    le_ref, est_ref, np_ref, nw_ref,
    pos_ref, noise_ref, posbuf, pbuf, jacc, grad, cc, kc, nuc, og, esum, lsum, erow, lrow, drift, dstage,
    sendbuf, recvbuf, moved, e0out, e0in, kept, arrived, wout, win, sumrow, sums_in, erows, erows_in, allrow, all_in, psum,
    aw_ref, awblock, blocks, possort, vtable, table, ts, tp, tn,
    ps, pr, ds_, dr, e0s, e0r, bs, br, ws, wr, ss, sr, es, er, gs, gr,
):
    gz = lax.axis_index("gz")
    gx = lax.axis_index("gx")
    gy = lax.axis_index("gy")
    me = gz * GY + gy
    rings = sorted(range(GY), key=lambda u: min(u, GY - u))
    arrival = [0, GY] + [u for dz in rings[1:] for u in (dz, GY + dz)]
    order = arrival[1:]

    def group_peer(u):
        z = lax.rem(gz + u // GY, GZ)
        y = lax.rem(gy + u % GY, GY)
        return z, y, z * GY + y

    def source_rank(u):
        z = lax.rem(gz + GZ - u // GY, GZ)
        return z * GY + lax.rem(gy + GY - u % GY, GY)

    def remote(src, dst, send, recv, peer):
        cp = pltpu.make_async_remote_copy(
            src_ref=src, dst_ref=dst, send_sem=send, recv_sem=recv,
            device_id=peer, device_id_type=pl.DeviceIdType.MESH,
        )
        cp.start()
        sent.append(cp)
        return cp

    sent = []
    pos_copy = pltpu.make_async_copy(pos_hbm, pos_ref, tp)
    pos_copy.start()
    noise_copy = pltpu.make_async_copy(noise_hbm, noise_ref, tn)
    noise_copy.start()
    barrier = pltpu.get_barrier_semaphore()
    for u in order:
        z, y, _ = group_peer(u)
        pl.semaphore_signal(barrier, inc=1, device_id=(z, gx, y), device_id_type=pl.DeviceIdType.MESH)
    for u in range(1, N_GX):
        pl.semaphore_signal(
            barrier, inc=1, device_id=(gz, lax.rem(gx + u, N_GX), gy), device_id_type=pl.DeviceIdType.MESH
        )
    exchange_tables(gx, source_ref, vtable)
    to_smem = pltpu.make_async_copy(vtable, table, ts)
    to_smem.start()
    constants(base_ref, disp_ref, charge_ref, decay_ref, coef_ref, cc, kc)
    esum[...] = jnp.zeros_like(esum)
    lsum[...] = jnp.zeros_like(lsum)
    lane_row = lax.broadcasted_iota(i32, (1, 128), 1)
    for b in range(BLOCKS):
        alive = jnp.where(lane_row < count_ref[b], 1.0, 0.0)
        awblock[b] = w_ref[b:b + 1, :] * alive
    pos_copy.wait()
    for b in range(BLOCKS):
        for c in range(3):
            blocks[b, c] = pos_ref[c, :, b * 128:(b + 1) * 128]
    to_smem.wait()

    def sort(j, _):
        possort[j] = blocks[table[8 + j, 0]]
        aw_ref[j] = awblock[table[8 + j, 0]]
        return 0

    lax.fori_loop(0, BLOCKS, sort, 0)
    for h in range(2):
        posbuf[h, :, 0:8, :] = possort[me * 2 + h]
        take_tile(h, 0, posbuf, pbuf)
    grad[...] = jnp.zeros_like(grad)
    psum[...] = jnp.zeros_like(psum)

    def geometries(at, first, last):
        def one(g, _):
            orbital_tiles(at, g, pbuf, cc, kc, og, esum, lsum)
            return 0

        lax.fori_loop(first, last, one, 0)

    pl.semaphore_wait(barrier, GROUP + N_GX - 2)

    pos_in = {}
    for h in range(2):
        for u in order:
            z, y, rank = group_peer(u)
            pos_in[u, h] = remote(
                possort.at[rank * 2 + h],
                posbuf.at[h, :, pl.ds(arrival.index(u) * 8, 8), :],
                ps.at[h, u], pr.at[h, u], (z, gx, y),
            )

    nuclear = repulsion(cc, kc, nuc)

    def arrive(h, k):
        pos_in[arrival[k], h].wait_recv()
        take_tile(h, k, posbuf, pbuf)

    def columns(h, first, last):
        def one(t, _):
            pair_column(h, t, pbuf, jacc, grad, psum)
            return 0

        lax.fori_loop(first, last, one, 0)

    base = []
    drift_in = [[], []]

    e0_in = []

    def early_energies():
        cross(0, grad, og, esum)
        for h in range(2):
            energy = jnp.sum(esum[0, h], axis=0, keepdims=True) + base[h]
            e0out[h:h + 1, :] = (energy + nuclear[0:1]) * (1.0 / NE)
        for u in order:
            z, y, _ = group_peer(u)
            e0_in.append(remote(e0out, e0in.at[me], e0s.at[u], e0r.at[u], (z, gx, y)))
        e0in[me] = e0out[...]

    def pairs(h):
        base.append(pair_end(h, pbuf, jacc, grad, psum))
        if h == 1:
            early_energies()
        for k in range(TILES):
            at = slice(k * 8, (k + 1) * 8)
            rank = source_rank(arrival[k])
            for c in range(3):
                drift[h, rank, c] = 0.2 * pbuf[h, c, at, :] + (
                    0.125 * grad[h, c, at, :] - 0.05 * og[0, h, c, at, :]
                )
        for u in order:
            z, y, rank = group_peer(u)
            drift_in[h].append(remote(
                drift.at[h, rank], dstage.at[me * 2 + h], ds_.at[h, u], dr.at[h, u], (z, gx, y)
            ))
        for c in range(3):
            dstage[me * 2 + h, c] = drift[h, me, c]

    geometries([(0, 0), (1, 0)], 0, G)
    for h in range(2):
        arrive(h, 1)
    geometries([(0, 1), (1, 1)], 0, G)
    for j in range(1, GY):
        arrive(0, 2 * j)
        arrive(0, 2 * j + 1)
        geometries([(0, 2 * j), (0, 2 * j + 1)], 0, G if j <= EARLY else 1)
        if j >= 4:
            columns(0, 2 * j, 2 * j + 2)
    columns(0, 1, 8)
    columns(0, 16, 17)
    pairs(0)
    for j in range(1, GY):
        arrive(1, 2 * j)
        arrive(1, 2 * j + 1)
        geometries([(1, 2 * j), (1, 2 * j + 1)], 0, 1)
    columns(1, 1, 17)
    pairs(1)

    rest = [(0, j) for j in range(EARLY + 1, GY)] + [(1, j) for j in range(1, GY)]
    blocks_in = []

    def pick(q, h, n):
        start = table[72 + q, 0]
        return jnp.minimum(start + lax.rem(start + h, 2) + 2 * n, BLOCKS - 1)

    def exchange_half(h):
        for cp in drift_in[h]:
            cp.wait_recv()

        def move(s, _):
            moved[s * 2 + h] = dstage[s * 2 + h] + 0.1 * blocks[table[8 + s * 2 + h, 0]]
            return 0

        lax.fori_loop(0, GROUP, move, 0)

        def pack(q, _):
            for n in range(2):
                sendbuf[h * BLOCKS + q * 2 + n] = moved[pick(q, h, n)]
            return 0

        lax.fori_loop(0, N_GX, pack, 0)
        for u in range(1, N_GX):
            q = lax.rem(gx + u, N_GX)
            blocks_in.append(remote(
                sendbuf.at[pl.ds(h * BLOCKS + q * 2, 2)], recvbuf.at[pl.ds(h * BLOCKS + gx * 2, 2)],
                bs.at[h, u], br.at[h, u], (gz, q, gy),
            ))
        for n in range(2):
            recvbuf[h * BLOCKS + gx * 2 + n] = sendbuf[h * BLOCKS + gx * 2 + n]

    for h, j in rest[:FIRST]:
        geometries([(h, 2 * j), (h, 2 * j + 1)], 1, G)
    noise_copy.wait()
    for b in range(BLOCKS):
        for c in range(3):
            blocks[b, c] = noise_ref[c, :, b * 128:(b + 1) * 128]
    exchange_half(0)
    for h, j in rest[FIRST:SECOND]:
        geometries([(h, 2 * j), (h, 2 * j + 1)], 1, G)
    for cp in e0_in:
        cp.wait_recv()
    for s in range(GROUP):
        for h in range(2):
            kept[2 * s + h, 0:1, :] = e0in[s, h:h + 1, :]
            kept[2 * s + h, 1:2, :] = aw_ref[2 * s + h]

    def packw(q, _):
        for h in range(2):
            for n in range(2):
                i = 2 * h + n
                wout[q, 2 * i:2 * i + 2, :] = kept[pick(q, h, n)][0:2]
        return 0

    lax.fori_loop(0, N_GX, packw, 0)
    w_in = []
    for u in range(1, N_GX):
        q = lax.rem(gx + u, N_GX)
        w_in.append(remote(wout.at[q], win.at[gx], ws.at[u], wr.at[u], (gz, q, gy)))
    win[gx] = wout[gx]
    for h, j in rest[SECOND:MIDDLE]:
        geometries([(h, 2 * j), (h, 2 * j + 1)], 1, G)
    exchange_half(1)

    for h, j in rest[MIDDLE:]:
        geometries([(h, 2 * j), (h, 2 * j + 1)], 1, G)
    lax.fori_loop(1, G, lambda g, _: (cross(g, grad, og, esum), 0)[1], 0)

    num = jnp.zeros((G, 128), f32)
    den = jnp.zeros((G, 128), f32)
    for h in range(2):
        for g in range(G):
            erow[h, g:g + 1, :] = jnp.sum(esum[g, h], axis=0, keepdims=True) + base[h]
            lrow[h, g:g + 1, :] = jnp.sum(lsum[g, h], axis=0, keepdims=True)
        le = (erow[h] + nuclear) * (1.0 / NE)
        logs = lrow[h]
        omega = aw_ref[me * 2 + h] * jnp.exp(2.0 * (logs - logs[0:1]))
        num = num + omega * le
        den = den + omega
        for z in range(GZ):
            erows[z, h] = le[z * HIGH:(z + 1) * HIGH]
    lane = lax.broadcasted_iota(i32, (G, 128), 1)
    sub = lax.broadcasted_iota(i32, (G, 128), 0)
    both = jnp.where(lane == sub, jnp.sum(num, axis=1, keepdims=True), 0.0) + jnp.where(
        lane == sub + G, jnp.sum(den, axis=1, keepdims=True), 0.0
    )
    sumrow[...] = jnp.sum(both, axis=0, keepdims=True)
    part_in = []
    rows_in = []
    for u in order:
        z, y, _ = group_peer(u)
        part_in.append(remote(sumrow, sums_in.at[me], ss.at[u], sr.at[u], (z, gx, y)))
    for u in order:
        z, y, _ = group_peer(u)
        rows_in.append(remote(erows.at[z], erows_in.at[pl.ds(me * 2, 2)], es.at[u], er.at[u], (z, gx, y)))
    sums_in[me] = sumrow[...]
    erows_in[pl.ds(me * 2, 2)] = erows[gz]
    for cp in part_in:
        cp.wait_recv()
    total = sums_in[0]
    for s in range(1, GROUP):
        total = total + sums_in[s]
    allrow[...] = total
    all_parts = []
    for u in range(1, N_GX):
        q = lax.rem(gx + u, N_GX)
        all_parts.append(remote(allrow, all_in.at[gx], gs.at[u], gr.at[u], (gz, q, gy)))
    all_in[gx] = allrow[...]
    for cp in rows_in:
        cp.wait_recv()
    for b in range(BLOCKS):
        le_ref[:, b * 128:(b + 1) * 128] = erows_in[table[40 + b, 0]]
    for cp in blocks_in:
        cp.wait_recv()
    for d in range(BLOCKS):
        block = recvbuf[table[gx // 4, lax.rem(gx, 4) * 32 + d]]
        for c in range(3):
            np_ref[c, :, d * 128:(d + 1) * 128] = block[c]
    for cp in w_in:
        cp.wait_recv()
    for q in range(N_GX):
        for h in range(2):
            for n in range(2):
                i = 2 * h + n
                arrived[h * BLOCKS + q * 2 + n, 0:2, :] = win[q, 2 * i:2 * i + 2, :]
    for cp in all_parts:
        cp.wait_recv()
    whole = all_in[0]
    for q in range(1, N_GX):
        whole = whole + all_in[q]
    estimate = whole / jnp.where(lane_row < G, pltpu.roll(whole, 128 - G, 1), 1.0)
    est_ref[...] = jnp.where(gz == 0, estimate, pltpu.roll(estimate, 128 - HIGH, 1))
    first = estimate[0:1, 0:1]
    for d in range(BLOCKS):
        pair = arrived[table[gx // 4, lax.rem(gx, 4) * 32 + d]]
        nw_ref[d:d + 1, :] = pair[1:2] * jnp.exp(first - pair[0:1])
    for cp in sent:
        cp.wait_send()


def local(
    positions, diffusion_noise, base_nuclei, displacements, charges, orbital_decay,
    coefficients, weights, counts, branch_source,
):
    vmem = pl.BlockSpec(memory_space=pltpu.VMEM)
    smem = pl.BlockSpec(memory_space=pltpu.SMEM)
    hbm = pl.BlockSpec(memory_space=pltpu.HBM)
    dma = pltpu.SemaphoreType.DMA
    v = lambda *shape: pltpu.VMEM(shape, f32)
    le, est, new_pos, new_w = pl.pallas_call(
        step_kernel,
        out_shape=(
            jax.ShapeDtypeStruct((HIGH, GROUP * 256), f32),
            jax.ShapeDtypeStruct((1, 128), f32),
            jax.ShapeDtypeStruct((3, 8, GROUP * 256), f32),
            jax.ShapeDtypeStruct((BLOCKS, BLK), f32),
        ),
        in_specs=[hbm, hbm, smem, smem, smem, smem, smem, vmem, smem, vmem],
        out_specs=(vmem,) * 4,
        scratch_shapes=[
            v(3, 8, GROUP * 256), v(3, 8, GROUP * 256), v(2, 3, 128, 128), v(2, 7, 256, 128),
            v(8, 3, 17 * 8, 128), v(2, 3, 128, 128), v(G, NA, 4, 8, 128), v(NA, 5, 8, 128), v(NA, 3, 8, 128),
            v(G, 2, 3, 128, 128), v(G, 2, 8, 128), v(G, 2, 8, 128), v(2, G, 128), v(2, G, 128),
            v(2, GROUP, 3, 8, 128), v(BLOCKS, 3, 8, 128), v(N_GX * CAP, 3, 8, 128), v(N_GX * CAP, 3, 8, 128),
            v(BLOCKS, 3, 8, 128), v(2, 128), v(GROUP, 2, 128), v(BLOCKS, 8, 128), v(N_GX * CAP, 8, 128),
            v(N_GX, 8, 128), v(N_GX, 8, 128), v(1, 128), v(GROUP, 1, 128), v(GZ, 2, HIGH, 128), v(BLOCKS, HIGH, 128),
            v(1, 128), v(N_GX, 1, 128), v(2, 2, 8, 128),
            v(BLOCKS, 1, BLK), v(BLOCKS, 1, BLK), v(BLOCKS, 3, 8, 128), v(BLOCKS, 3, 8, 128),
            pltpu.VMEM((88, 128), i32), pltpu.SMEM((88, 128), i32), dma, dma, dma,
            dma((2, GROUP)), dma((2, GROUP)), dma((2, GROUP)), dma((2, GROUP)), dma((GROUP,)), dma((GROUP,)),
            dma((2, N_GX)), dma((2, N_GX)), dma((N_GX,)), dma((N_GX,)), dma((GROUP,)), dma((GROUP,)),
            dma((GROUP,)), dma((GROUP,)), dma((N_GX,)), dma((N_GX,)),
        ],
        compiler_params=pltpu.CompilerParams(
            collective_id=0, has_side_effects=True, vmem_limit_bytes=67043328
        ),
    )(
        positions.transpose(1, 0, 2), diffusion_noise.transpose(1, 0, 2), base_nuclei.T, displacements.transpose(2, 0, 1),
        charges, orbital_decay, coefficients, weights.reshape(BLOCKS, BLK), counts,
        branch_source.reshape(4, 128),
    )
    le, est, new_pos, new_w = pl.pallas_call(
        finish_kernel,
        out_shape=(
            jax.ShapeDtypeStruct(le.shape, f32), jax.ShapeDtypeStruct((HIGH,), f32),
            jax.ShapeDtypeStruct(new_pos.shape, f32), jax.ShapeDtypeStruct(new_w.shape, f32),
        ),
        in_specs=[vmem, smem, vmem, vmem],
        out_specs=(vmem, smem, vmem, vmem),
    )(le, est, new_pos, new_w)
    return le, est, new_pos.transpose(1, 0, 2), new_w.reshape(-1)


def solution(mesh):
    placed = (
        P(("gz", "gy"), None, "gx"), P(("gz", "gy"), None, "gx"), P(), P(), P(), P(), P(),
        P("gx"), P("gx"), P(),
    )
    return jax.shard_map(
        local,
        mesh=mesh,
        in_specs=placed,
        out_specs=(P("gz", "gx"), P("gz"), P(("gz", "gy"), None, "gx"), P("gx")),
        check_vma=False,
    )
```
